32 devices in a mesh: bank: 4 (over x, core), lane: 8 (over z, y).
Axes of the slice: x: 2, y: 2, z: 4, core: 2. Of those that a mesh axis runs over, the one named last changes fastest.
Arguments:
- amplitudes: float32 [2, 256, 128, 128], P(None, ('bank', 'lane')), may hold values from -6 to 6
- energies: float32 [256, 128, 128], P(('bank', 'lane')), may hold values from -2 to 2
- diagonal_angles: float32 [2, 128], replicated, may hold values from 0.3 to 1.2
Outputs:
- final_parts: float32 [2, 256, 128, 128], P(None, ('bank', 'lane'))
- marginal: float32 [64, 128, 128], P('lane', 'bank')
The draws below stay inside these ranges and needn't reach their ends.
All inputs are finite; a program needn't handle non-finite values.
Results may differ from the reference program's by a relative error of at most 0.0003.
Values sent between devices are 32-bit elements; how exact they have to be, the bound alone decides.
A program may use at most 64 MiB of HBM per device.

```python
import jax
import jax.numpy as jnp
from jax import lax

BLOCKS_DEV = 8
ROWS = 128
LANES = 128
BLOCKS = 256
LAYERS = 2
N_BANK = 4
N_LANE = 8


def block_scale(stream_key, dims, pieces, smallest, high):
    loudness, own = 1.0, jax.random.fold_in(stream_key, 6)
    for position, blocks in pieces:
        heights = jnp.exp(jax.random.uniform(jax.random.fold_in(own, position), (blocks,), jnp.float32, smallest / len(pieces), high / len(pieces)))
        loudness = loudness * jnp.repeat(heights, dims[position] // blocks).reshape([-1 if axis == position else 1 for axis in range(len(dims))])
    return loudness


def normal_values(key, shape, width, most, shards=(), held_as=jnp.bfloat16):
    drawn = width * jax.random.normal(key, shape, jnp.float32)
    if shards:
        drawn = drawn * block_scale(key, shape, shards, -0.22, 0.18)
    return jnp.clip(drawn, -most, most).astype(held_as)


def setup_inputs(seed: int = 0) -> dict:
    splits = jax.random.split(jax.random.key(seed), 4)
    return {
        "amplitudes": normal_values(splits[0], (2, BLOCKS, ROWS, LANES), 1.0, 6.0, ((1, 32),), jnp.float32),
        "energies": jnp.clip(jax.random.uniform(splits[1], (BLOCKS, ROWS, LANES), jnp.float32, -2.0, 2.0) * block_scale(splits[1], (BLOCKS, ROWS, LANES), ((0, 32),), -0.4, 0.0), -2.0, 2.0),
        "diagonal_angles": jnp.clip(jax.random.uniform(splits[2], (LAYERS, LANES), jnp.float32, 0.3, 1.2), 0.3, 1.2),
    }


def count_bits(values, count):
    places = jnp.arange(count.bit_length() - 1, dtype=jnp.int32)
    return jnp.sum((values[..., None] >> places) & 1, axis=-1)


def walsh_table(count):
    rank = jnp.arange(count, dtype=jnp.int32)
    parity = count_bits(rank[:, None] & rank[None, :], count) % 2
    real_part = jnp.where(parity == 1, -1.0, 1.0).astype(jnp.float32) * (count ** -0.5)
    return real_part


def apply_along(values, dim):
    real_part = walsh_table(values.shape[dim])
    def times(table):
        moved = jnp.tensordot(values, table, axes=([dim], [0]), precision=lax.Precision.HIGHEST)
        return jnp.moveaxis(moved, -1, dim)
    return times(real_part)


def diagonal_step(values, levels, angle):
    turn = angle * levels
    return jnp.stack([values[0] * jnp.cos(turn) + values[1] * jnp.sin(turn), values[1] * jnp.cos(turn) - values[0] * jnp.sin(turn)])


def reference(amplitudes, energies, diagonal_angles):
    values = amplitudes
    for layer in range(LAYERS):
        values = diagonal_step(values, energies, diagonal_angles[layer])
        values = apply_along(values, 3)
        values = apply_along(values, 2)
        parts = values.reshape(2, N_BANK, N_LANE, BLOCKS_DEV, ROWS, LANES)
        parts = apply_along(parts, 1)
        parts = apply_along(parts, 2)
        parts = apply_along(parts, 3)
        values = parts.reshape(values.shape)
    chance = values[0] * values[0] + values[1] * values[1]
    marginal = jnp.mean(chance.reshape(N_BANK, -1, ROWS, LANES), axis=0)
    return values, marginal
```

```python
import functools

import jax
import jax.numpy as jnp
import numpy as np
from jax import lax
from jax.experimental import pallas as pl
from jax.experimental.pallas import tpu as pltpu
from jax.sharding import PartitionSpec as P

MESH = pl.DeviceIdType.MESH
TABLE = 256
SUB = 8


def walsh_table():
    rank = np.arange(TABLE)
    both = rank[:, None] & rank[None, :]
    parity = sum((both >> place) & 1 for place in range(8)) % 2
    return jnp.asarray(np.where(parity == 1, -1.0, 1.0) / 16.0, jnp.bfloat16)


def cos_sin(turn):
    half = turn * 0.5
    x = half * half
    s = -1.0 / 39916800.0
    for term in (1.0 / 362880.0, -1.0 / 5040.0, 1.0 / 120.0, -1.0 / 6.0, 1.0):
        s = s * x + term
    s = s * half
    c = 1.0 / 479001600.0
    for term in (-1.0 / 3628800.0, 1.0 / 40320.0, -1.0 / 720.0, 1.0 / 24.0, -0.5, 1.0):
        c = c * x + term
    return 1.0 - 2.0 * (s * s), 2.0 * (s * c)


def split(values):
    high = values.astype(jnp.bfloat16)
    return high, (values - high.astype(jnp.float32)).astype(jnp.bfloat16)


def mix(items):
    items, step = list(items), 1
    while step < len(items):
        for low in range(len(items)):
            if not low & step:
                u, v = items[low], items[low + step]
                items[low], items[low + step] = u + v, u - v
        step *= 2
    return items


def dot(a, b):
    return jnp.dot(a, b, preferred_element_type=jnp.float32)


def mix_lanes(values, table):
    high, low = split(values)
    return dot(jnp.concatenate([high, low], axis=1), table[:, :128])


def kernel(
    n_bank, n_lane, chunks,
    a_hbm, e_hbm, angle_hbm, table_hbm,
    out_ref, marginal_ref,
    a_ref, e_ref, angle_ref, table_ref,
    held, sent1, got1, sent2, got2, levels, cosine, sine, chance, chances,
    in_sem, e_send, e_recv, send1, recv1, send2, recv2, m_send, m_recv,
):
    devices = n_bank * n_lane
    _, blocks, rows, lanes = a_ref.shape
    group = blocks * rows // devices
    groups = rows // group
    bank, lane = lax.axis_index("bank"), lax.axis_index("lane")
    me = bank * n_lane + lane

    fetches = [
        pltpu.make_async_copy(src, dst, in_sem.at[i])
        for i, (src, dst) in enumerate([
            (e_hbm, e_ref), (a_hbm, a_ref), (angle_hbm, angle_ref), (table_hbm, table_ref),
        ])
    ]
    for fetch in fetches:
        fetch.start()

    def others(act):
        low = lane < n_lane // 2

        def around(step, _):
            pair = step - lax.rem(step, 2)
            there = jnp.where(low, n_lane - 2 - pair, pair) + lax.rem(step + lane, 2)
            for turn in range(1, n_bank):
                act(lax.rem(bank + turn, n_bank), there)

            @pl.when(there != lane)
            def _():
                act(bank, there)

            return 0

        lax.fori_loop(0, n_lane, around, 0)

    barrier = pltpu.get_barrier_semaphore()

    def greet(to_bank, to_lane):
        pl.semaphore_signal(
            barrier, inc=1, device_id=(to_bank, to_lane), device_id_type=MESH
        )

    others(greet)
    fetches[0].wait()
    pl.semaphore_wait(barrier, devices - 1)

    def swap(src, dst, send_sem, recv_sem):
        def one(to_bank, to_lane):
            pltpu.make_async_remote_copy(
                src_ref=src.at[to_bank * n_lane + to_lane], dst_ref=dst.at[me],
                send_sem=send_sem, recv_sem=recv_sem,
                device_id=(to_bank, to_lane), device_id_type=MESH,
            ).start()

        others(one)

    def arrive(buffer, sem):
        most = buffer.at[pl.ds(0, devices - 1)]
        pltpu.make_async_copy(most, most, sem).wait()

    swap(e_ref, levels, e_send, e_recv)
    levels[me] = e_ref[me]
    for fetch in fetches[1:]:
        fetch.wait()

    table = table_ref[...]

    def block_step(b, _):
        first = b * groups
        level = e_ref[pl.ds(first, groups)].reshape(rows, lanes)
        c, s = cos_sin(level * angle_ref[0:1, :])
        re, im = a_ref[0, b], a_ref[1, b]
        turned = jnp.concatenate([re * c + im * s, im * c - re * s], axis=0)
        along = mix_lanes(turned, table)
        high, low = split(jnp.concatenate([along[:rows], along[rows:]], axis=1))
        mixed = dot(table[:128, :], jnp.concatenate([high, low], axis=0))
        held[b, 0] = mixed[:, :lanes]
        held[b, 1] = mixed[:, lanes:]
        return 0

    lax.fori_loop(0, blocks, block_step, 0)

    for chunk in range(chunks):
        def spread(g, _, chunk=chunk):
            start = pl.multiple_of(g * group + chunk * SUB, SUB)
            for part in range(2):
                mixed = mix([held[b, part, pl.ds(start, SUB), :] for b in range(blocks)])
                for b in range(blocks):
                    sent1[chunk, b * groups + g, part] = mixed[b]
            return 0

        lax.fori_loop(0, groups, spread, 0)
        swap(sent1.at[chunk], got1.at[chunk], send1.at[chunk], recv1.at[chunk])
        got1[chunk, me] = sent1[chunk, me]

    arrive(levels, e_recv)

    def phases(d, _):
        c, s = cos_sin(levels[d] * angle_ref[1:2, :])
        cosine[d] = c
        sine[d] = s
        return 0

    lax.fori_loop(0, devices, phases, 0)

    def send_back(chunk):
        swap(sent2.at[chunk], got2.at[chunk], send2.at[chunk], recv2.at[chunk])
        got2[chunk, me] = sent2[chunk, me]

    wide = TABLE // SUB
    half = max(chunks // 2, 1)
    for chunk in range(chunks):
        arrive(got1.at[chunk], recv1.at[chunk])
        there = pl.ds(chunk * SUB, SUB)
        re = mix([got1[chunk, d, 0] for d in range(devices)])
        im = mix([got1[chunk, d, 1] for d in range(devices)])
        done = []
        for start in range(0, devices, wide):
            r, i = [], []
            for d in range(start, start + wide):
                c, s = cosine[d, there, :], sine[d, there, :]
                r.append(re[d] * c + im[d] * s)
                i.append(im[d] * c - re[d] * s)
            along = mix_lanes(jnp.concatenate(r + i, axis=0), table)
            pair = jnp.concatenate([along[:TABLE], along[TABLE:]], axis=1)
            high, low = split(pair)
            done.append(dot(table, high) + dot(table, low))
        done = mix(done)
        first = chunk - chunk % half
        last = chunk % half == half - 1
        for d in range(devices):
            at = d % wide * SUB
            for part in range(2):
                tile = done[d // wide][at : at + SUB, part * lanes : (part + 1) * lanes]
                if last:
                    tiles = mix([sent2[c, d, part] for c in range(first, chunk)] + [tile])
                    for c in range(half):
                        sent2[first + c, d, part] = tiles[c]
                else:
                    sent2[chunk, d, part] = tile
        if last:
            send_back(first)

    for chunk in range(1, half):
        def halves(d, _, chunk=chunk):
            for part in range(2):
                u, v = sent2[chunk, d, part], sent2[chunk + half, d, part]
                sent2[chunk, d, part] = u + v
                sent2[chunk + half, d, part] = u - v
            return 0

        lax.fori_loop(0, devices, halves, 0)

    scale = float(TABLE * TABLE) / (devices * blocks * rows * lanes)
    share = rows // n_bank // group
    steps = [(0, half)] if chunks > 1 else [(0,)]
    steps += [(c,) for first in range(1, half) for c in (first, first + half)]
    queue = [c for step in steps[1:] for c in step]
    if queue:
        send_back(queue.pop(0))

    def back(chunk, part):
        return mix([got2[chunk, d, part] for d in range(devices)])

    copies = {}
    for step in steps:
        for chunk in step[:-1]:
            arrive(got2.at[chunk], recv2.at[chunk])
            for part in range(2):
                mixed = back(chunk, part)
                for d in range(devices):
                    got2[chunk, d, part] = mixed[d]
        arrive(got2.at[step[-1]], recv2.at[step[-1]])
        for part in range(2):
            mixed = back(step[-1], part)
            for d in range(devices):
                tiles = mix([got2[c, d, part] for c in step[:-1]] + [mixed[d]])
                b, g = divmod(d, groups)
                for chunk, tile in zip(step, tiles):
                    value = tile * scale
                    at = g * group + chunk * SUB
                    out_ref[part, b, at : at + SUB, :] = value
                    spot = (chunk, g // share, b, pl.ds(g % share * SUB, SUB))
                    square = value * value
                    chance[spot] = chance[spot] + square if part else square
        for chunk in step:
            copies[chunk] = []
            for turn in range(1, n_bank):
                other = lax.rem(bank + turn, n_bank)
                copies[chunk].append(pltpu.make_async_remote_copy(
                    src_ref=chance.at[chunk, other], dst_ref=chances.at[chunk, turn - 1],
                    send_sem=m_send.at[chunk, turn - 1], recv_sem=m_recv.at[chunk, turn - 1],
                    device_id=(other, lane), device_id_type=MESH,
                ))
                copies[chunk][-1].start()
        if queue:
            send_back(queue.pop(0))
    for step in steps:
        for chunk in step:
            for copy in copies[chunk]:
                copy.wait_recv()
            total = chance[chunk, bank]
            for turn in range(1, n_bank):
                total = total + chances[chunk, turn - 1]
            total = total * (1.0 / n_bank)
            for g in range(share):
                at = g * group + chunk * SUB
                marginal_ref[:, at : at + SUB, :] = total[:, g * SUB : (g + 1) * SUB]

    for chunk in range(chunks):
        for copy in copies[chunk]:
            copy.wait_send()
    arrive(e_ref, e_send)
    for chunk in range(chunks):
        arrive(sent1.at[chunk], send1.at[chunk])
        arrive(sent2.at[chunk], send2.at[chunk])


def put_out(state_ref, marginal_ref, state_out, marginal_out, sem):
    copies = [
        pltpu.make_async_copy(state_ref, state_out, sem.at[0]),
        pltpu.make_async_copy(marginal_ref, marginal_out, sem.at[1]),
    ]
    for copy in copies:
        copy.start()
    for copy in copies:
        copy.wait()


def shards(n_bank, n_lane, amplitudes, energies, angles):
    devices = n_bank * n_lane
    _, blocks, rows, lanes = amplitudes.shape
    group = blocks * rows // devices
    chunks = group // SUB
    f32 = jnp.float32
    table = walsh_table()
    whole = pl.BlockSpec(memory_space=pltpu.VMEM)
    swapped = pltpu.VMEM((chunks, devices, 2, SUB, lanes), f32)
    real = pltpu.VMEM((devices, group, lanes), f32)
    strip = (blocks, rows // n_bank, lanes)
    part = (blocks, rows // n_bank // chunks, lanes)
    one, many = pltpu.SemaphoreType.DMA, pltpu.SemaphoreType.DMA((chunks,))
    state, marginal = pl.pallas_call(
        functools.partial(kernel, n_bank, n_lane, chunks),
        out_shape=(
            pltpu.VMEM(amplitudes.shape, f32),
            pltpu.VMEM(strip, f32),
        ),
        in_specs=[pl.BlockSpec(memory_space=pltpu.HBM)] * 4,
        out_specs=(whole, whole),
        scratch_shapes=[
            pltpu.VMEM(amplitudes.shape, f32),
            real,
            pltpu.VMEM(angles.shape, f32),
            pltpu.VMEM(table.shape, table.dtype),
            pltpu.VMEM((blocks, 2, rows, lanes), f32),
            swapped, swapped, swapped, swapped,
            real, real, real,
            pltpu.VMEM((chunks, n_bank, *part), f32),
            pltpu.VMEM((chunks, n_bank - 1, *part), f32),
            pltpu.SemaphoreType.DMA((4,)),
            one, one, many, many, many, many,
            pltpu.SemaphoreType.DMA((chunks, n_bank - 1)),
            pltpu.SemaphoreType.DMA((chunks, n_bank - 1)),
        ],
        compiler_params=pltpu.CompilerParams(
            collective_id=0, has_side_effects=True
        ),
        name="walsh",
    )(amplitudes, energies.reshape(devices, group, lanes), angles, table)
    return pl.pallas_call(
        put_out,
        out_shape=(
            jax.ShapeDtypeStruct(state.shape, f32),
            jax.ShapeDtypeStruct(marginal.shape, f32),
        ),
        in_specs=[whole] * 2,
        out_specs=(pl.BlockSpec(memory_space=pltpu.HBM),) * 2,
        scratch_shapes=[pltpu.SemaphoreType.DMA((2,))],
        compiler_params=pltpu.CompilerParams(vmem_limit_bytes=1024 * 1024),
        name="put_out",
    )(state, marginal)


def solution(mesh):
    sizes = mesh.shape
    return jax.shard_map(
        functools.partial(shards, sizes["bank"], sizes["lane"]),
        mesh=mesh,
        in_specs=(P(None, ("bank", "lane"), None, None), P(("bank", "lane"), None, None), P()),
        out_specs=(P(None, ("bank", "lane"), None, None), P("lane", "bank", None)),
        check_vma=False,
    )
```

```python
import functools

import jax
import jax.numpy as jnp
from jax import lax
from jax.experimental import pallas as pl
from jax.experimental.pallas import tpu as pltpu
from jax.sharding import PartitionSpec as P

MESH = pl.DeviceIdType.MESH
TABLE = 256
SUB = 8
HALF = SUB // 2
PLANES = 4


def walsh_table():
    both = lax.broadcasted_iota(jnp.int32, (TABLE, TABLE), 0)
    both = both & lax.broadcasted_iota(jnp.int32, (TABLE, TABLE), 1)
    for place in (4, 2, 1):
        both = both ^ (both >> place)
    sign = 1 - 2 * (both & 1)
    return (sign.astype(jnp.float32) * (1.0 / 16.0)).astype(jnp.bfloat16)


def cos_sin(turn):
    half = turn * 0.5
    x = half * half
    s = -1.0 / 39916800.0
    for term in (1.0 / 362880.0, -1.0 / 5040.0, 1.0 / 120.0, -1.0 / 6.0, 1.0):
        s = s * x + term
    s = s * half
    c = 1.0 / 479001600.0
    for term in (-1.0 / 3628800.0, 1.0 / 40320.0, -1.0 / 720.0, 1.0 / 24.0, -0.5, 1.0):
        c = c * x + term
    return 1.0 - 2.0 * (s * s), 2.0 * (s * c)


def split(values):
    high = values.astype(jnp.bfloat16)
    return high, (values - high.astype(jnp.float32)).astype(jnp.bfloat16)


def mix(items):
    items, step = list(items), 1
    while step < len(items):
        for low in range(len(items)):
            if not low & step:
                u, v = items[low], items[low + step]
                items[low], items[low + step] = u + v, u - v
        step *= 2
    return items


def dot(a, b):
    return jnp.dot(a, b, preferred_element_type=jnp.float32)


def mix_lanes(values, table):
    high, low = split(values)
    return dot(jnp.concatenate([high, low], axis=1), table[:, :128])


def kernel(
    n_bank, n_lane, chunks,
    a_hbm, e_hbm, angle_hbm,
    out_ref, marginal_ref,
    a_ref, e_ref, angle_ref, table_ref,
    held, sent1, got1, sent2, got2, levels, cosine, sine,
    chance, chances, thin_chance, thin_chances,
    in_sem, e_send, e_recv, send1, recv1, send2, recv2, m_send, m_recv,
):
    devices = n_bank * n_lane
    _, blocks, rows, lanes = a_ref.shape
    group = blocks * rows // devices
    groups = rows // group
    bank, lane = lax.axis_index("bank"), lax.axis_index("lane")
    me = bank * n_lane + lane

    fetches = [
        pltpu.make_async_copy(src, dst, in_sem.at[i])
        for i, (src, dst) in enumerate([
            (e_hbm, e_ref), (a_hbm, a_ref), (angle_hbm, angle_ref),
        ])
    ]
    for fetch in fetches:
        fetch.start()

    deep = n_lane // PLANES
    lower = lane < n_lane // 2
    plane = lane // deep
    outer = (plane == 0) | (plane == PLANES - 1)

    def to_plane(far, act):
        first = jnp.where(lower, PLANES - 1 - far, far) * deep

        def around(step, _):
            there = first + lax.rem(step + lane, deep)
            for turn in range(1, n_bank):
                act(lax.rem(bank + turn, n_bank), there)
            if far < PLANES // 2:
                act(bank, there)
            else:
                pl.when(there != lane)(lambda: act(bank, there))
            return 0

        lax.fori_loop(0, deep, around, 0)

    def others(act):
        for far in range(PLANES):
            to_plane(far, act)

    barrier = pltpu.get_barrier_semaphore()

    def greet(to_bank, to_lane):
        pl.semaphore_signal(
            barrier, inc=1, device_id=(to_bank, to_lane), device_id_type=MESH
        )

    others(greet)
    table_ref[...] = walsh_table()
    fetches[0].wait()
    pl.semaphore_wait(barrier, devices - 1)

    def give(src, dst, send_sem, recv_sem, to_bank, to_lane, spot=()):
        pltpu.make_async_remote_copy(
            src_ref=src.at[(to_bank * n_lane + to_lane, *spot)], dst_ref=dst.at[(me, *spot)],
            send_sem=send_sem, recv_sem=recv_sem,
            device_id=(to_bank, to_lane), device_id_type=MESH,
        ).start()

    def swap(*ends):
        others(functools.partial(give, *ends))

    def arrive(buffer, sem, spot=()):
        most = buffer.at[(pl.ds(0, devices - 1), *spot)]
        pltpu.make_async_copy(most, most, sem).wait()

    swap(e_ref, levels, e_send, e_recv)
    levels[me] = e_ref[me]
    for fetch in fetches[1:]:
        fetch.wait()

    table = table_ref[...]

    def block_step(b, _):
        first = b * groups
        level = e_ref[pl.ds(first, groups)].reshape(rows, lanes)
        c, s = cos_sin(level * angle_ref[0:1, :])
        re, im = a_ref[0, b], a_ref[1, b]
        turned = jnp.concatenate([re * c + im * s, im * c - re * s], axis=0)
        along = mix_lanes(turned, table)
        high, low = split(jnp.concatenate([along[:rows], along[rows:]], axis=1))
        mixed = dot(table[:128, :], jnp.concatenate([high, low], axis=0))
        held[b, 0] = mixed[:, :lanes]
        held[b, 1] = mixed[:, lanes:]
        return 0

    lax.fori_loop(0, blocks, block_step, 0)

    for chunk in range(chunks):
        def spread(g, _, chunk=chunk):
            start = pl.multiple_of(g * group + chunk * SUB, SUB)
            for part in range(2):
                mixed = mix([held[b, part, pl.ds(start, SUB), :] for b in range(blocks)])
                for b in range(blocks):
                    sent1[chunk, b * groups + g, part] = mixed[b]
            return 0

        lax.fori_loop(0, groups, spread, 0)
        swap(sent1.at[chunk], got1.at[chunk], send1.at[chunk], recv1.at[chunk])
        got1[chunk, me] = sent1[chunk, me]

    arrive(levels, e_recv)

    def phases(d, _):
        c, s = cos_sin(levels[d] * angle_ref[1:2, :])
        cosine[d] = c
        sine[d] = s
        return 0

    lax.fori_loop(0, devices, phases, 0)

    wide = TABLE // SUB
    half = max(chunks // 2, 1)
    thin = chunks - 1 if half > 1 else chunks
    messages = [(c, ()) for c in range(thin)]
    messages += [(c, (h,)) for c in range(thin, chunks) for h in range(2)]

    def give_back(at, far):
        chunk, spot = messages[at]
        ends = sent2.at[chunk], got2.at[chunk], send2.at[at], recv2.at[at]
        to_plane(far, lambda b, l: give(*ends, b, l, spot))

    def send_back(order):
        for at, far in order:
            give_back(at, far)
        for at in sorted({at for at, _ in order}):
            chunk, spot = messages[at]
            got2[(chunk, me, *spot)] = sent2[(chunk, me, *spot)]

    def far_first(*those):
        return [(at, far) for at in those for far in range(PLANES)]

    def take_back(at):
        chunk, spot = messages[at]
        arrive(got2.at[chunk], recv2.at[at], spot)

    for chunk in range(chunks):
        arrive(got1.at[chunk], recv1.at[chunk])
        if chunk == chunks - 1 > 0:
            pl.when(outer)(lambda: send_back(far_first(0)))
        there = pl.ds(chunk * SUB, SUB)
        re = mix([got1[chunk, d, 0] for d in range(devices)])
        im = mix([got1[chunk, d, 1] for d in range(devices)])
        done = []
        for start in range(0, devices, wide):
            r, i = [], []
            for d in range(start, start + wide):
                c, s = cosine[d, there, :], sine[d, there, :]
                r.append(re[d] * c + im[d] * s)
                i.append(im[d] * c - re[d] * s)
            along = mix_lanes(jnp.concatenate(r + i, axis=0), table)
            pair = jnp.concatenate([along[:TABLE], along[TABLE:]], axis=1)
            high, low = split(pair)
            done.append(dot(table, high) + dot(table, low))
        done = mix(done)
        first = chunk - chunk % half
        last = chunk % half == half - 1
        for d in range(devices):
            at = d % wide * SUB
            for part in range(2):
                tile = done[d // wide][at : at + SUB, part * lanes : (part + 1) * lanes]
                if last:
                    tiles = mix([sent2[c, d, part] for c in range(first, chunk)] + [tile])
                    for c in range(half):
                        sent2[first + c, d, part] = tiles[c]
                else:
                    sent2[chunk, d, part] = tile
        if last and first == chunk + 1 - chunks:
            send_back(far_first(first))
        elif last and first == 0:
            pl.when(jnp.logical_not(outer))(lambda: send_back(far_first(0)))
        elif last:
            send_back(far_first(first))

    for chunk in range(1, half):
        def halves(d, _, chunk=chunk):
            differ = []
            for part in range(2):
                u, v = sent2[chunk, d, part], sent2[chunk + half, d, part]
                sent2[chunk, d, part] = u + v
                differ.append(u - v)
            for h in range(2):
                tile = differ[h]
                if chunk + half == thin:
                    rows_h = slice(h * HALF, (h + 1) * HALF)
                    tile = jnp.concatenate([part[rows_h] for part in differ], axis=0)
                sent2[chunk + half, d, h] = tile
            return 0

        lax.fori_loop(0, devices, halves, 0)

    scale = float(TABLE * TABLE) / (devices * blocks * rows * lanes)
    share = rows // n_bank // group
    steps = [(0, half)] if chunks > 1 else [(0,)]
    steps += [(c,) for first in range(1, half) for c in (first, first + half)]
    steps[-1:] = [(at,) for at in range(thin, len(messages))] or steps[-1:]
    if len(messages) > chunks:
        send_back(far_first(*[at for (at,) in steps[1:-3]]))
        x, y, z = [at for (at,) in steps[-3:]]
        order = [(x, 0), (y, 0), (z, 0), (x, 1), (y, 1), (z, 1)]
        send_back(order + [(at, far) for at in (x, y, z) for far in (2, 3)])

    def back(chunk, part):
        return mix([got2[chunk, d, part] for d in range(devices)])

    def whole(step):
        for chunk in step[:-1]:
            take_back(chunk)
            for part in range(2):
                mixed = back(chunk, part)
                for d in range(devices):
                    got2[chunk, d, part] = mixed[d]
        take_back(step[-1])
        for part in range(2):
            mixed = back(step[-1], part)
            for d in range(devices):
                tiles = mix([got2[c, d, part] for c in step[:-1]] + [mixed[d]])
                b, g = divmod(d, groups)
                for chunk, tile in zip(step, tiles):
                    value = tile * scale
                    at = g * group + chunk * SUB
                    out_ref[part, b, at : at + SUB, :] = value
                    spot = (chunk, g // share, b, pl.ds(g % share * SUB, SUB))
                    square = value * value
                    chance[spot] = chance[spot] + square if part else square

    def thinner(at):
        take_back(at)
        chunk, (h,) = messages[at]
        mixed = back(chunk, h)
        for d in range(devices):
            b, g = divmod(d, groups)
            value = mixed[d] * scale
            row = g * group + chunk * SUB + h * HALF
            for part in range(2):
                out_ref[part, b, row : row + HALF, :] = value[part * HALF : (part + 1) * HALF]
            square = value * value
            low, high = b % few, b // few
            spot = (h, g // share, low, pl.ds(g % share * SUB + high * HALF, HALF))
            thin_chance[spot] = square[:HALF] + square[HALF:]

    few = blocks // 2
    copies = {}
    for step in steps:
        if step[0] < thin:
            whole(step)
        else:
            thinner(step[0])
        for at in step:
            src, dst, place = chance, chances, at
            if at >= thin:
                src, dst, place = thin_chance, thin_chances, at - thin
            copies[at] = []
            for turn in range(1, n_bank):
                other = lax.rem(bank + turn, n_bank)
                copies[at].append(pltpu.make_async_remote_copy(
                    src_ref=src.at[place, other], dst_ref=dst.at[place, turn - 1],
                    send_sem=m_send.at[at, turn - 1], recv_sem=m_recv.at[at, turn - 1],
                    device_id=(other, lane), device_id_type=MESH,
                ))
                copies[at][-1].start()
    for step in steps:
        for at in step:
            for copy in copies[at]:
                copy.wait_recv()
            src, dst, place = chance, chances, at
            if at >= thin:
                src, dst, place = thin_chance, thin_chances, at - thin
            total = src[place, bank]
            for turn in range(1, n_bank):
                total = total + dst[place, turn - 1]
            total = total * (1.0 / n_bank)
            for g in range(share):
                row = g * group + messages[at][0] * SUB
                if at < thin:
                    marginal_ref[:, row : row + SUB, :] = total[:, g * SUB : (g + 1) * SUB]
                else:
                    row = row + place * HALF
                    for high in range(2):
                        from_row = g * SUB + high * HALF
                        marginal_ref[high * few : (high + 1) * few, row : row + HALF, :] = (
                            total[:, from_row : from_row + HALF]
                        )

    for at in range(len(messages)):
        for copy in copies[at]:
            copy.wait_send()
    arrive(e_ref, e_send)
    for chunk in range(chunks):
        arrive(sent1.at[chunk], send1.at[chunk])
    for at, (chunk, spot) in enumerate(messages):
        arrive(sent2.at[chunk], send2.at[at], spot)


def put_out(state_ref, marginal_ref, state_out, marginal_out, sem):
    copies = [
        pltpu.make_async_copy(state_ref, state_out, sem.at[0]),
        pltpu.make_async_copy(marginal_ref, marginal_out, sem.at[1]),
    ]
    for copy in copies:
        copy.start()
    for copy in copies:
        copy.wait()


def shards(n_bank, n_lane, amplitudes, energies, angles):
    devices = n_bank * n_lane
    _, blocks, rows, lanes = amplitudes.shape
    group = blocks * rows // devices
    chunks = group // SUB
    f32 = jnp.float32
    whole = pl.BlockSpec(memory_space=pltpu.VMEM)
    swapped = pltpu.VMEM((chunks, devices, 2, SUB, lanes), f32)
    real = pltpu.VMEM((devices, group, lanes), f32)
    strip = (blocks, rows // n_bank, lanes)
    part = (blocks, rows // n_bank // chunks, lanes)
    thin = (blocks // 2, rows // n_bank // chunks, lanes)
    one, many = pltpu.SemaphoreType.DMA, pltpu.SemaphoreType.DMA((chunks,))
    more = pltpu.SemaphoreType.DMA((chunks + 1,))
    state, marginal = pl.pallas_call(
        functools.partial(kernel, n_bank, n_lane, chunks),
        out_shape=(
            pltpu.VMEM(amplitudes.shape, f32),
            pltpu.VMEM(strip, f32),
        ),
        in_specs=[pl.BlockSpec(memory_space=pltpu.HBM)] * 3,
        out_specs=(whole, whole),
        scratch_shapes=[
            pltpu.VMEM(amplitudes.shape, f32),
            real,
            pltpu.VMEM(angles.shape, f32),
            pltpu.VMEM((TABLE, TABLE), jnp.bfloat16),
            pltpu.VMEM((blocks, 2, rows, lanes), f32),
            swapped, swapped, swapped, swapped,
            real, real, real,
            pltpu.VMEM((chunks, n_bank, *part), f32),
            pltpu.VMEM((chunks, n_bank - 1, *part), f32),
            pltpu.VMEM((2, n_bank, *thin), f32),
            pltpu.VMEM((2, n_bank - 1, *thin), f32),
            pltpu.SemaphoreType.DMA((3,)),
            one, one, many, many, more, more,
            pltpu.SemaphoreType.DMA((chunks + 1, n_bank - 1)),
            pltpu.SemaphoreType.DMA((chunks + 1, n_bank - 1)),
        ],
        compiler_params=pltpu.CompilerParams(
            collective_id=0, has_side_effects=True
        ),
        name="walsh",
    )(amplitudes, energies.reshape(devices, group, lanes), angles)
    return pl.pallas_call(
        put_out,
        out_shape=(
            jax.ShapeDtypeStruct(state.shape, f32),
            jax.ShapeDtypeStruct(marginal.shape, f32),
        ),
        in_specs=[whole] * 2,
        out_specs=(pl.BlockSpec(memory_space=pltpu.HBM),) * 2,
        scratch_shapes=[pltpu.SemaphoreType.DMA((2,))],
        compiler_params=pltpu.CompilerParams(vmem_limit_bytes=1024 * 1024),
        name="put_out",
    )(state, marginal)


def solution(mesh):
    sizes = mesh.shape
    return jax.shard_map(
        functools.partial(shards, sizes["bank"], sizes["lane"]),
        mesh=mesh,
        in_specs=(P(None, ("bank", "lane"), None, None), P(("bank", "lane"), None, None), P()),
        out_specs=(P(None, ("bank", "lane"), None, None), P("lane", "bank", None)),
        check_vma=False,
    )
```

```python
import functools

import jax
import jax.numpy as jnp
from jax import lax
from jax.experimental import pallas as pl
from jax.experimental.pallas import tpu as pltpu
from jax.sharding import PartitionSpec as P

MESH = pl.DeviceIdType.MESH
TABLE = 256
SUB = 8
HALF = SUB // 2
PLANES = 4


def walsh_table():
    both = lax.broadcasted_iota(jnp.int32, (TABLE, TABLE), 0)
    both = both & lax.broadcasted_iota(jnp.int32, (TABLE, TABLE), 1)
    for place in (4, 2, 1):
        both = both ^ (both >> place)
    sign = 1 - 2 * (both & 1)
    return (sign.astype(jnp.float32) * (1.0 / 16.0)).astype(jnp.bfloat16)


def cos_sin(turn):
    half = turn * 0.5
    x = half * half
    s = -1.0 / 39916800.0
    for term in (1.0 / 362880.0, -1.0 / 5040.0, 1.0 / 120.0, -1.0 / 6.0, 1.0):
        s = s * x + term
    s = s * half
    c = 1.0 / 479001600.0
    for term in (-1.0 / 3628800.0, 1.0 / 40320.0, -1.0 / 720.0, 1.0 / 24.0, -0.5, 1.0):
        c = c * x + term
    return 1.0 - 2.0 * (s * s), 2.0 * (s * c)


def split(values):
    high = values.astype(jnp.bfloat16)
    return high, (values - high.astype(jnp.float32)).astype(jnp.bfloat16)


def mix(items):
    items, step = list(items), 1
    while step < len(items):
        for low in range(len(items)):
            if not low & step:
                u, v = items[low], items[low + step]
                items[low], items[low + step] = u + v, u - v
        step *= 2
    return items


def dot(a, b):
    return jnp.dot(a, b, preferred_element_type=jnp.float32)


def mix_lanes(values, table):
    high, low = split(values)
    return dot(jnp.concatenate([high, low], axis=1), table[:, :128])


def kernel(
    n_bank, n_lane, chunks,
    a_hbm, e_hbm, angle_hbm,
    out_ref, marginal_ref,
    a_ref, e_ref, angle_ref, table_ref,
    held, sent1, got1, sent2, got2, levels, cosine, sine,
    chance, chances, thin_chance, thin_chances,
    in_sem, e_send, e_recv, send1, recv1, send2, recv2, m_send, m_recv, known,
):
    devices = n_bank * n_lane
    _, blocks, rows, lanes = a_ref.shape
    group = blocks * rows // devices
    groups = rows // group
    bank, lane = lax.axis_index("bank"), lax.axis_index("lane")
    me = bank * n_lane + lane

    fetches = [
        pltpu.make_async_copy(src, dst, in_sem.at[i])
        for i, (src, dst) in enumerate([
            (e_hbm, e_ref), (a_hbm, a_ref), (angle_hbm, angle_ref),
        ])
    ]
    for fetch in fetches:
        fetch.start()

    deep = n_lane // PLANES
    lower = lane < n_lane // 2
    plane = lane // deep
    outer = (plane == 0) | (plane == PLANES - 1)

    def to_plane(far, act):
        first = jnp.where(lower, PLANES - 1 - far, far) * deep

        def around(step, _):
            there = first + lax.rem(step + lane + 1, deep)
            for turn in range(1, n_bank):
                act(lax.rem(bank + turn, n_bank), there)
            if far < PLANES // 2:
                act(bank, there)
            else:
                pl.when(there != lane)(lambda: act(bank, there))
            return 0

        lax.fori_loop(0, deep, around, 0)

    def others(act):
        for far in range(PLANES):
            to_plane(far, act)

    barrier = pltpu.get_barrier_semaphore()

    def greet(to_bank, to_lane):
        pl.semaphore_signal(
            barrier, inc=1, device_id=(to_bank, to_lane), device_id_type=MESH
        )

    next_lane = (plane + 1 - 2 * lax.rem(plane, 2)) * deep + lax.rem(lane, deep)
    mirror_lane = (PLANES - 1 - plane) * deep + lax.rem(lane, deep)

    def tell(step, to_lane):
        pl.semaphore_signal(
            known.at[step], inc=1, device_id=(bank, to_lane), device_id_type=MESH
        )

    @pl.when(outer)
    def _():
        greet(bank, next_lane)
        to_plane(3, greet)

    @pl.when(jnp.logical_not(outer))
    def _():
        to_plane(1, greet)
        greet(bank, next_lane)
        to_plane(2, greet)

    table_ref[...] = walsh_table()
    fetches[0].wait()

    def give(src, dst, send_sem, recv_sem, to_bank, to_lane, spot=()):
        pltpu.make_async_remote_copy(
            src_ref=src.at[(to_bank * n_lane + to_lane, *spot)], dst_ref=dst.at[(me, *spot)],
            send_sem=send_sem, recv_sem=recv_sem,
            device_id=(to_bank, to_lane), device_id_type=MESH,
        ).start()

    def swap(*ends):
        others(functools.partial(give, *ends))

    def arrive(buffer, sem, spot=()):
        most = buffer.at[(pl.ds(0, devices - 1), *spot)]
        pltpu.make_async_copy(most, most, sem).wait()

    give_e = functools.partial(give, e_ref, levels, e_send, e_recv)

    @pl.when(outer)
    def _():
        pl.semaphore_wait(barrier, n_bank * deep)
        tell(0, next_lane)
        to_plane(3, give_e)
        pl.semaphore_wait(known.at[0], 1)
        to_plane(1, give_e)
        to_plane(2, give_e)
        pl.semaphore_wait(known.at[2], 1)
        to_plane(0, give_e)

    @pl.when(jnp.logical_not(outer))
    def _():
        pl.semaphore_wait(barrier, 2 * n_bank * deep)
        tell(0, next_lane)
        to_plane(1, give_e)
        to_plane(2, give_e)
        pl.semaphore_wait(known.at[0], 1)
        tell(1, mirror_lane)
        to_plane(3, give_e)
        pl.semaphore_wait(known.at[1], 1)
        tell(2, next_lane)
        to_plane(0, give_e)

    levels[me] = e_ref[me]
    for fetch in fetches[1:]:
        fetch.wait()

    table = table_ref[...]

    def block_step(b, _):
        first = b * groups
        level = e_ref[pl.ds(first, groups)].reshape(rows, lanes)
        c, s = cos_sin(level * angle_ref[0:1, :])
        re, im = a_ref[0, b], a_ref[1, b]
        turned = jnp.concatenate([re * c + im * s, im * c - re * s], axis=0)
        along = mix_lanes(turned, table)
        high, low = split(jnp.concatenate([along[:rows], along[rows:]], axis=1))
        mixed = dot(table[:128, :], jnp.concatenate([high, low], axis=0))
        held[b, 0] = mixed[:, :lanes]
        held[b, 1] = mixed[:, lanes:]
        return 0

    lax.fori_loop(0, blocks, block_step, 0)

    for chunk in range(chunks):
        def spread(g, _, chunk=chunk):
            start = pl.multiple_of(g * group + chunk * SUB, SUB)
            for part in range(2):
                mixed = mix([held[b, part, pl.ds(start, SUB), :] for b in range(blocks)])
                for b in range(blocks):
                    sent1[chunk, b * groups + g, part] = mixed[b]
            return 0

        lax.fori_loop(0, groups, spread, 0)
        swap(sent1.at[chunk], got1.at[chunk], send1.at[chunk], recv1.at[chunk])
        got1[chunk, me] = sent1[chunk, me]

    arrive(levels, e_recv)

    def phases(d, _):
        c, s = cos_sin(levels[d] * angle_ref[1:2, :])
        cosine[d] = c
        sine[d] = s
        return 0

    lax.fori_loop(0, devices, phases, 0)

    wide = TABLE // SUB
    half = max(chunks // 2, 1)
    thin = (half - 1, chunks - 1) if half > 1 else ()
    fat = [c for c in range(chunks) if c not in thin]
    messages = [(c, ()) for c in fat] + [(c, (h,)) for c in thin for h in range(2)]
    few = blocks // 2

    def give_back(at, far):
        chunk, spot = messages[at]
        ends = sent2.at[chunk], got2.at[chunk], send2.at[at], recv2.at[at]
        to_plane(far, lambda b, l: give(*ends, b, l, spot))

    def send_back(order):
        for at, far in order:
            give_back(at, far)
        for at in sorted({at for at, _ in order}):
            chunk, spot = messages[at]
            got2[(chunk, me, *spot)] = sent2[(chunk, me, *spot)]

    def far_first(*those):
        return [(at, far) for at in those for far in range(PLANES)]

    def take_back(at):
        chunk, spot = messages[at]
        arrive(got2.at[chunk], recv2.at[at], spot)

    for chunk in range(chunks):
        arrive(got1.at[chunk], recv1.at[chunk])
        if chunk == chunks - 1 > 0:
            pl.when(outer)(lambda: send_back(far_first(0)))
        there = pl.ds(chunk * SUB, SUB)
        re = mix([got1[chunk, d, 0] for d in range(devices)])
        im = mix([got1[chunk, d, 1] for d in range(devices)])
        done = []
        for start in range(0, devices, wide):
            r, i = [], []
            for d in range(start, start + wide):
                c, s = cosine[d, there, :], sine[d, there, :]
                r.append(re[d] * c + im[d] * s)
                i.append(im[d] * c - re[d] * s)
            along = mix_lanes(jnp.concatenate(r + i, axis=0), table)
            pair = jnp.concatenate([along[:TABLE], along[TABLE:]], axis=1)
            high, low = split(pair)
            done.append(dot(table, high) + dot(table, low))
        done = mix(done)
        first = chunk - chunk % half
        last = chunk % half == half - 1
        for d in range(devices):
            at = d % wide * SUB
            for part in range(2):
                tile = done[d // wide][at : at + SUB, part * lanes : (part + 1) * lanes]
                if last:
                    tiles = mix([sent2[c, d, part] for c in range(first, chunk)] + [tile])
                    for c in range(half):
                        sent2[first + c, d, part] = tiles[c]
                else:
                    sent2[chunk, d, part] = tile
        if last and first == chunk + 1 - chunks:
            send_back(far_first(0))
        elif last and first == 0:
            pl.when(jnp.logical_not(outer))(lambda: send_back(far_first(0)))
        elif last:
            send_back(far_first(fat.index(first)))

    for chunk in range(1, half):
        def halves(d, _, chunk=chunk):
            u, v = sent2[chunk, d], sent2[chunk + half, d]
            for to, both in ((chunk, u + v), (chunk + half, u - v)):
                if to in thin:
                    both = [
                        jnp.concatenate([part[h * HALF : (h + 1) * HALF] for part in both])
                        for h in range(2)
                    ]
                for i in range(2):
                    sent2[to, d, i] = both[i]
            return 0

        lax.fori_loop(0, devices, halves, 0)

    scale = float(TABLE * TABLE) / (devices * blocks * rows * lanes)
    share = rows // n_bank // group
    slim = list(range(len(fat), len(messages)))
    steps = [(0, fat.index(half))] if chunks > 1 else [(0,)]
    for first in range(1, half - 1):
        steps += [(fat.index(c),) for c in (first, first + half)]
        send_back(far_first(*steps[-2], *steps[-1]))
    steps += [(at,) for at in slim]
    send_back([(at, far) for at in slim for far in (2, 3)] + [(at, far) for far in (0, 1) for at in slim])

    def back(chunk, part):
        return mix([got2[chunk, d, part] for d in range(devices)])

    def whole(step):
        places = [messages[at][0] for at in step]
        for at, chunk in zip(step[:-1], places):
            take_back(at)
            for part in range(2):
                mixed = back(chunk, part)
                for d in range(devices):
                    got2[chunk, d, part] = mixed[d]
        take_back(step[-1])
        for part in range(2):
            mixed = back(places[-1], part)
            for d in range(devices):
                tiles = mix([got2[c, d, part] for c in places[:-1]] + [mixed[d]])
                b, g = divmod(d, groups)
                for at, chunk, tile in zip(step, places, tiles):
                    value = tile * scale
                    row = g * group + chunk * SUB
                    out_ref[part, b, row : row + SUB, :] = value
                    spot = (at, g // share, b, pl.ds(g % share * SUB, SUB))
                    square = value * value
                    chance[spot] = chance[spot] + square if part else square

    def thinner(at):
        take_back(at)
        chunk, (h,) = messages[at]
        mixed = back(chunk, h)
        for d in range(devices):
            b, g = divmod(d, groups)
            value = mixed[d] * scale
            row = g * group + chunk * SUB + h * HALF
            for part in range(2):
                out_ref[part, b, row : row + HALF, :] = value[part * HALF : (part + 1) * HALF]
            square = value * value
            low, high = b % few, b // few
            spot = (at - len(fat), g // share, low, pl.ds(g % share * SUB + high * HALF, HALF))
            thin_chance[spot] = square[:HALF] + square[HALF:]

    copies = {}
    for step in steps:
        if step[0] < len(fat):
            whole(step)
        else:
            thinner(step[0])
        for at in step:
            src, dst, place = chance, chances, at
            if at >= len(fat):
                src, dst, place = thin_chance, thin_chances, at - len(fat)
            copies[at] = []
            for turn in range(1, n_bank):
                other = lax.rem(bank + turn, n_bank)
                copies[at].append(pltpu.make_async_remote_copy(
                    src_ref=src.at[place, other], dst_ref=dst.at[place, turn - 1],
                    send_sem=m_send.at[at, turn - 1], recv_sem=m_recv.at[at, turn - 1],
                    device_id=(other, lane), device_id_type=MESH,
                ))
                copies[at][-1].start()
    for step in steps:
        for at in step:
            for copy in copies[at]:
                copy.wait_recv()
            src, dst, place = chance, chances, at
            if at >= len(fat):
                src, dst, place = thin_chance, thin_chances, at - len(fat)
            total = src[place, bank]
            for turn in range(1, n_bank):
                total = total + dst[place, turn - 1]
            total = total * (1.0 / n_bank)
            chunk, spot = messages[at]
            for g in range(share):
                row = g * group + chunk * SUB
                if not spot:
                    marginal_ref[:, row : row + SUB, :] = total[:, g * SUB : (g + 1) * SUB]
                    continue
                row = row + spot[0] * HALF
                for high in range(2):
                    at_row = g * SUB + high * HALF
                    marginal_ref[high * few : (high + 1) * few, row : row + HALF, :] = (
                        total[:, at_row : at_row + HALF]
                    )

    for at in range(len(messages)):
        for copy in copies[at]:
            copy.wait_send()
    arrive(e_ref, e_send)
    for chunk in range(chunks):
        arrive(sent1.at[chunk], send1.at[chunk])
    for at, (chunk, spot) in enumerate(messages):
        arrive(sent2.at[chunk], send2.at[at], spot)


def put_out(state_ref, marginal_ref, state_out, marginal_out, sem):
    copies = [
        pltpu.make_async_copy(state_ref, state_out, sem.at[0]),
        pltpu.make_async_copy(marginal_ref, marginal_out, sem.at[1]),
    ]
    for copy in copies:
        copy.start()
    for copy in copies:
        copy.wait()


def shards(n_bank, n_lane, amplitudes, energies, angles):
    devices = n_bank * n_lane
    _, blocks, rows, lanes = amplitudes.shape
    group = blocks * rows // devices
    chunks = group // SUB
    f32 = jnp.float32
    whole = pl.BlockSpec(memory_space=pltpu.VMEM)
    swapped = pltpu.VMEM((chunks, devices, 2, SUB, lanes), f32)
    real = pltpu.VMEM((devices, group, lanes), f32)
    strip = (blocks, rows // n_bank, lanes)
    part = (blocks, rows // n_bank // chunks, lanes)
    thin = (blocks // 2, rows // n_bank // chunks, lanes)
    n_thin = 4 if chunks > 2 else 0
    n_fat = chunks - n_thin // 2
    n_messages = n_fat + n_thin
    one, many = pltpu.SemaphoreType.DMA, pltpu.SemaphoreType.DMA((chunks,))
    more = pltpu.SemaphoreType.DMA((n_messages,))
    state, marginal = pl.pallas_call(
        functools.partial(kernel, n_bank, n_lane, chunks),
        out_shape=(
            pltpu.VMEM(amplitudes.shape, f32),
            pltpu.VMEM(strip, f32),
        ),
        in_specs=[pl.BlockSpec(memory_space=pltpu.HBM)] * 3,
        out_specs=(whole, whole),
        scratch_shapes=[
            pltpu.VMEM(amplitudes.shape, f32),
            real,
            pltpu.VMEM(angles.shape, f32),
            pltpu.VMEM((TABLE, TABLE), jnp.bfloat16),
            pltpu.VMEM((blocks, 2, rows, lanes), f32),
            swapped, swapped, swapped, swapped,
            real, real, real,
            pltpu.VMEM((n_fat, n_bank, *part), f32),
            pltpu.VMEM((n_fat, n_bank - 1, *part), f32),
            pltpu.VMEM((max(n_thin, 1), n_bank, *thin), f32),
            pltpu.VMEM((max(n_thin, 1), n_bank - 1, *thin), f32),
            pltpu.SemaphoreType.DMA((3,)),
            one, one, many, many, more, more,
            pltpu.SemaphoreType.DMA((n_messages, n_bank - 1)),
            pltpu.SemaphoreType.DMA((n_messages, n_bank - 1)),
            pltpu.SemaphoreType.REGULAR((3,)),
        ],
        compiler_params=pltpu.CompilerParams(
            collective_id=0, has_side_effects=True
        ),
        name="walsh",
    )(amplitudes, energies.reshape(devices, group, lanes), angles)
    return pl.pallas_call(
        put_out,
        out_shape=(
            jax.ShapeDtypeStruct(state.shape, f32),
            jax.ShapeDtypeStruct(marginal.shape, f32),
        ),
        in_specs=[whole] * 2,
        out_specs=(pl.BlockSpec(memory_space=pltpu.HBM),) * 2,
        scratch_shapes=[pltpu.SemaphoreType.DMA((2,))],
        compiler_params=pltpu.CompilerParams(vmem_limit_bytes=1024 * 1024),
        name="put_out",
    )(state, marginal)


def solution(mesh):
    sizes = mesh.shape
    return jax.shard_map(
        functools.partial(shards, sizes["bank"], sizes["lane"]),
        mesh=mesh,
        in_specs=(P(None, ("bank", "lane"), None, None), P(("bank", "lane"), None, None), P()),
        out_specs=(P(None, ("bank", "lane"), None, None), P("lane", "bank", None)),
        check_vma=False,
    )
```

```python
import functools

import jax
import jax.numpy as jnp
from jax import lax
from jax.experimental import pallas as pl
from jax.experimental.pallas import tpu as pltpu
from jax.sharding import PartitionSpec as P

MESH = pl.DeviceIdType.MESH
TABLE = 256
SUB = 8
HALF = SUB // 2
PLANES = 4


def walsh_table():
    both = lax.broadcasted_iota(jnp.int32, (TABLE, TABLE), 0)
    both = both & lax.broadcasted_iota(jnp.int32, (TABLE, TABLE), 1)
    for place in (4, 2, 1):
        both = both ^ (both >> place)
    sign = 1 - 2 * (both & 1)
    return (sign.astype(jnp.float32) * (1.0 / 16.0)).astype(jnp.bfloat16)


def cos_sin(turn):
    half = turn * 0.5
    x = half * half
    s = -1.0 / 39916800.0
    for term in (1.0 / 362880.0, -1.0 / 5040.0, 1.0 / 120.0, -1.0 / 6.0, 1.0):
        s = s * x + term
    s = s * half
    c = 1.0 / 479001600.0
    for term in (-1.0 / 3628800.0, 1.0 / 40320.0, -1.0 / 720.0, 1.0 / 24.0, -0.5, 1.0):
        c = c * x + term
    return 1.0 - 2.0 * (s * s), 2.0 * (s * c)


def split(values):
    high = values.astype(jnp.bfloat16)
    return high, (values - high.astype(jnp.float32)).astype(jnp.bfloat16)


def mix(items):
    items, step = list(items), 1
    while step < len(items):
        for low in range(len(items)):
            if not low & step:
                u, v = items[low], items[low + step]
                items[low], items[low + step] = u + v, u - v
        step *= 2
    return items


def dot(a, b):
    return jnp.dot(a, b, preferred_element_type=jnp.float32)


def mix_lanes(values, table):
    high, low = split(values)
    return dot(jnp.concatenate([high, low], axis=1), table[:, :128])


def kernel(
    n_bank, n_lane, chunks,
    a_hbm, e_hbm, angle_hbm,
    out_ref, marginal_ref,
    a_ref, e_ref, angle_ref, table_ref,
    held, sent1, got1, sent2, got2, levels, cosine, sine,
    chance, chances, thin_chance, thin_chances,
    in_sem, sent, e_recv, recv1, recv2, m_recv, known,
):
    devices = n_bank * n_lane
    _, blocks, rows, lanes = a_ref.shape
    group = blocks * rows // devices
    groups = rows // group
    bank, lane = lax.axis_index("bank"), lax.axis_index("lane")
    me = bank * n_lane + lane

    fetches = [
        pltpu.make_async_copy(src, dst, in_sem.at[i])
        for i, (src, dst) in enumerate([
            (e_hbm, e_ref), (a_hbm, a_ref), (angle_hbm, angle_ref),
        ])
    ]
    for fetch in fetches:
        fetch.start()

    deep = n_lane // PLANES
    lower = lane < n_lane // 2
    plane = lane // deep
    outer = (plane == 0) | (plane == PLANES - 1)

    def to_plane(far, act):
        first = jnp.where(lower, PLANES - 1 - far, far) * deep

        def around(step, _):
            there = first + lax.rem(step + lane + 1, deep)
            for turn in range(1, n_bank):
                act(lax.rem(bank + turn, n_bank), there)
            if far < PLANES // 2:
                act(bank, there)
            else:
                pl.when(there != lane)(lambda: act(bank, there))
            return 0

        lax.fori_loop(0, deep, around, 0)

    def to_mirror(corner, act):
        first = (PLANES - 1 - plane) * deep
        pair = n_bank // 2
        opposite = lax.rem(bank // pair + 1, 2) * pair

        def around(step, _):
            there = first + lax.rem(step + lane, deep)
            for turn in range(pair):
                act(opposite + turn, there)
            return 0

        def beside(step, _):
            there = first + lax.rem(step + lane, deep)
            for turn in range(pair):
                act(bank // pair * pair + lax.rem(bank + turn, pair), there)
            return 0

        if corner:
            lax.fori_loop(1, deep, around, 0)
        else:
            lax.fori_loop(0, deep, beside, 0)
            around(0, 0)

    def others(act):
        for far in range(PLANES):
            to_plane(far, act)

    barrier = pltpu.get_barrier_semaphore()

    def greet(to_bank, to_lane):
        pl.semaphore_signal(
            barrier, inc=1, device_id=(to_bank, to_lane), device_id_type=MESH
        )

    next_lane = (plane + 1 - 2 * lax.rem(plane, 2)) * deep + lax.rem(lane, deep)
    mirror_lane = (PLANES - 1 - plane) * deep + lax.rem(lane, deep)

    def tell(step, to_lane):
        pl.semaphore_signal(
            known.at[step], inc=1, device_id=(bank, to_lane), device_id_type=MESH
        )

    @pl.when(outer)
    def _():
        greet(bank, next_lane)
        to_plane(3, greet)

    @pl.when(jnp.logical_not(outer))
    def _():
        to_plane(2, greet)
        to_mirror(False, greet)
        greet(bank, next_lane)

    table_ref[...] = walsh_table()
    fetches[0].wait()

    def give(src, dst, send_sem, recv_sem, to_bank, to_lane, spot=()):
        pltpu.make_async_remote_copy(
            src_ref=src.at[(to_bank * n_lane + to_lane, *spot)], dst_ref=dst.at[(me, *spot)],
            send_sem=send_sem, recv_sem=recv_sem,
            device_id=(to_bank, to_lane), device_id_type=MESH,
        ).start()

    def swap(*ends):
        others(functools.partial(give, *ends))

    def wait_for(buffer, sem):
        pltpu.make_async_copy(buffer, buffer, sem).wait()

    def arrive(buffer, sem, spot=()):
        wait_for(buffer.at[(pl.ds(0, devices - 1), *spot)], sem)

    give_e = functools.partial(give, e_ref, levels, sent.at[0], e_recv)

    @pl.when(outer)
    def _():
        pl.semaphore_wait(barrier, n_bank * deep)
        tell(0, next_lane)
        to_plane(3, give_e)
        pl.semaphore_wait(known.at[0], 1)
        to_plane(1, give_e)
        to_plane(2, give_e)
        pl.semaphore_wait(known.at[2], 1)
        to_plane(0, give_e)

    @pl.when(jnp.logical_not(outer))
    def _():
        pl.semaphore_wait(barrier, 2 * n_bank * deep - n_bank // 2 * (deep - 1))
        tell(3, mirror_lane)
        to_mirror(False, give_e)
        to_plane(2, give_e)
        pl.semaphore_wait(known.at[3], 1)
        tell(0, next_lane)
        to_mirror(True, give_e)
        pl.semaphore_wait(known.at[0], 1)
        tell(1, mirror_lane)
        to_plane(3, give_e)
        pl.semaphore_wait(known.at[1], 1)
        tell(2, next_lane)
        to_plane(0, give_e)

    levels[me] = e_ref[me]
    for fetch in fetches[1:]:
        fetch.wait()

    table = table_ref[...]

    def block_step(b, _):
        first = b * groups
        level = e_ref[pl.ds(first, groups)].reshape(rows, lanes)
        c, s = cos_sin(level * angle_ref[0:1, :])
        re, im = a_ref[0, b], a_ref[1, b]
        turned = jnp.concatenate([re * c + im * s, im * c - re * s], axis=0)
        along = mix_lanes(turned, table)
        high, low = split(jnp.concatenate([along[:rows], along[rows:]], axis=1))
        mixed = dot(table[:128, :], jnp.concatenate([high, low], axis=0))
        held[b, 0] = mixed[:, :lanes]
        held[b, 1] = mixed[:, lanes:]
        return 0

    lax.fori_loop(0, blocks, block_step, 0)

    for chunk in range(chunks):
        def spread(g, _, chunk=chunk):
            start = pl.multiple_of(g * group + chunk * SUB, SUB)
            for part in range(2):
                mixed = mix([held[b, part, pl.ds(start, SUB), :] for b in range(blocks)])
                for b in range(blocks):
                    sent1[chunk, b * groups + g, part] = mixed[b]
            return 0

        lax.fori_loop(0, groups, spread, 0)
        swap(sent1.at[chunk], got1.at[chunk], sent.at[1], recv1.at[chunk])
        got1[chunk, me] = sent1[chunk, me]

    arrive(levels, e_recv)

    def phases(d, _):
        c, s = cos_sin(levels[d] * angle_ref[1:2, :])
        cosine[d] = c
        sine[d] = s
        return 0

    lax.fori_loop(0, devices, phases, 0)

    wide = TABLE // SUB
    half = max(chunks // 2, 1)
    thin = (half - 1, chunks - 1) if half > 1 else ()
    fat = [c for c in range(chunks) if c not in thin]
    messages = [(c, ()) for c in fat] + [(c, (h,)) for c in thin for h in range(2)]
    few = blocks // 2

    def give_back(at, far):
        chunk, spot = messages[at]
        ends = sent2.at[chunk], got2.at[chunk], sent.at[2], recv2.at[at]
        to_plane(far, lambda b, l: give(*ends, b, l, spot))

    def send_back(order):
        for at, far in order:
            give_back(at, far)
        for at in sorted({at for at, _ in order}):
            chunk, spot = messages[at]
            got2[(chunk, me, *spot)] = sent2[(chunk, me, *spot)]

    def far_first(*those):
        return [(at, far) for at in those for far in range(PLANES)]

    def take_back(at):
        chunk, spot = messages[at]
        arrive(got2.at[chunk], recv2.at[at], spot)

    for chunk in range(chunks):
        arrive(got1.at[chunk], recv1.at[chunk])
        if chunk == chunks - 1 > 0:
            pl.when(outer)(lambda: send_back(far_first(0)))
        there = pl.ds(chunk * SUB, SUB)
        re = mix([got1[chunk, d, 0] for d in range(devices)])
        im = mix([got1[chunk, d, 1] for d in range(devices)])
        done = []
        for start in range(0, devices, wide):
            r, i = [], []
            for d in range(start, start + wide):
                c, s = cosine[d, there, :], sine[d, there, :]
                r.append(re[d] * c + im[d] * s)
                i.append(im[d] * c - re[d] * s)
            along = mix_lanes(jnp.concatenate(r + i, axis=0), table)
            pair = jnp.concatenate([along[:TABLE], along[TABLE:]], axis=1)
            high, low = split(pair)
            done.append(dot(table, high) + dot(table, low))
        done = mix(done)
        first = chunk - chunk % half
        last = chunk % half == half - 1
        for d in range(devices):
            at = d % wide * SUB
            for part in range(2):
                tile = done[d // wide][at : at + SUB, part * lanes : (part + 1) * lanes]
                if last:
                    tiles = mix([sent2[c, d, part] for c in range(first, chunk)] + [tile])
                    for c in range(half):
                        sent2[first + c, d, part] = tiles[c]
                else:
                    sent2[chunk, d, part] = tile
        if last and first == chunk + 1 - chunks:
            send_back(far_first(0))
        elif last and first == 0:
            pl.when(jnp.logical_not(outer))(lambda: send_back(far_first(0)))
        elif last:
            send_back(far_first(fat.index(first)))

    for chunk in range(1, half):
        def halves(d, _, chunk=chunk):
            u, v = sent2[chunk, d], sent2[chunk + half, d]
            for to, both in ((chunk, u + v), (chunk + half, u - v)):
                if to in thin:
                    both = [
                        jnp.concatenate([part[h * HALF : (h + 1) * HALF] for part in both])
                        for h in range(2)
                    ]
                for i in range(2):
                    sent2[to, d, i] = both[i]
            return 0

        lax.fori_loop(0, devices, halves, 0)

    scale = float(TABLE * TABLE) / (devices * blocks * rows * lanes)
    share = rows // n_bank // group
    slim = list(range(len(fat), len(messages)))
    steps = [(0, fat.index(half))] if chunks > 1 else [(0,)]
    for first in range(1, half - 1):
        steps += [(fat.index(c),) for c in (first, first + half)]
        send_back(far_first(*steps[-2], *steps[-1]))
    steps += [(at,) for at in slim]
    send_back([(at, far) for at in slim for far in (2, 3)] + [(at, far) for far in (0, 1) for at in slim])

    def back(chunk, part):
        return mix([got2[chunk, d, part] for d in range(devices)])

    def whole(step):
        places = [messages[at][0] for at in step]
        for at, chunk in zip(step[:-1], places):
            take_back(at)
            for part in range(2):
                mixed = back(chunk, part)
                for d in range(devices):
                    got2[chunk, d, part] = mixed[d]
        take_back(step[-1])
        for part in range(2):
            mixed = back(places[-1], part)
            for d in range(devices):
                tiles = mix([got2[c, d, part] for c in places[:-1]] + [mixed[d]])
                b, g = divmod(d, groups)
                for at, chunk, tile in zip(step, places, tiles):
                    value = tile * scale
                    row = g * group + chunk * SUB
                    out_ref[part, b, row : row + SUB, :] = value
                    spot = (at, g // share, b, pl.ds(g % share * SUB, SUB))
                    square = value * value
                    chance[spot] = chance[spot] + square if part else square

    def thinner(at):
        take_back(at)
        chunk, (h,) = messages[at]
        mixed = back(chunk, h)
        for d in range(devices):
            b, g = divmod(d, groups)
            value = mixed[d] * scale
            row = g * group + chunk * SUB + h * HALF
            for part in range(2):
                out_ref[part, b, row : row + HALF, :] = value[part * HALF : (part + 1) * HALF]
            square = value * value
            low, high = b % few, b // few
            spot = (at - len(fat), g // share, low, pl.ds(g % share * SUB + high * HALF, HALF))
            thin_chance[spot] = square[:HALF] + square[HALF:]

    for step in steps:
        if step[0] < len(fat):
            whole(step)
        else:
            thinner(step[0])
        for at in step:
            src, dst, place, group_sem = chance, chances, at, 3
            if at >= len(fat):
                src, dst, place, group_sem = thin_chance, thin_chances, at - len(fat), 4
            for turn in range(1, n_bank):
                other = lax.rem(bank + turn, n_bank)
                pltpu.make_async_remote_copy(
                    src_ref=src.at[place, other], dst_ref=dst.at[place, turn - 1],
                    send_sem=sent.at[group_sem], recv_sem=m_recv.at[at],
                    device_id=(other, lane), device_id_type=MESH,
                ).start()
    for step in steps:
        for at in step:
            src, dst, place = chance, chances, at
            if at >= len(fat):
                src, dst, place = thin_chance, thin_chances, at - len(fat)
            wait_for(dst.at[place], m_recv.at[at])
            total = src[place, bank]
            for turn in range(1, n_bank):
                total = total + dst[place, turn - 1]
            total = total * (1.0 / n_bank)
            chunk, spot = messages[at]
            for g in range(share):
                row = g * group + chunk * SUB
                if not spot:
                    marginal_ref[:, row : row + SUB, :] = total[:, g * SUB : (g + 1) * SUB]
                    continue
                row = row + spot[0] * HALF
                for high in range(2):
                    at_row = g * SUB + high * HALF
                    marginal_ref[high * few : (high + 1) * few, row : row + HALF, :] = (
                        total[:, at_row : at_row + HALF]
                    )

    wait_for(chances, sent.at[3])
    if slim:
        wait_for(thin_chances, sent.at[4])
    arrive(e_ref, sent.at[0])
    wait_for(sent1.at[:, pl.ds(0, devices - 1)], sent.at[1])
    wait_for(sent2.at[:, pl.ds(0, devices - 1)], sent.at[2])


def put_out(state_ref, marginal_ref, state_out, marginal_out, sem):
    copies = [
        pltpu.make_async_copy(state_ref, state_out, sem.at[0]),
        pltpu.make_async_copy(marginal_ref, marginal_out, sem.at[1]),
    ]
    for copy in copies:
        copy.start()
    for copy in copies:
        copy.wait()


def shards(n_bank, n_lane, amplitudes, energies, angles):
    devices = n_bank * n_lane
    _, blocks, rows, lanes = amplitudes.shape
    group = blocks * rows // devices
    chunks = group // SUB
    f32 = jnp.float32
    whole = pl.BlockSpec(memory_space=pltpu.VMEM)
    swapped = pltpu.VMEM((chunks, devices, 2, SUB, lanes), f32)
    real = pltpu.VMEM((devices, group, lanes), f32)
    strip = (blocks, rows // n_bank, lanes)
    part = (blocks, rows // n_bank // chunks, lanes)
    thin = (blocks // 2, rows // n_bank // chunks, lanes)
    n_thin = 4 if chunks > 2 else 0
    n_fat = chunks - n_thin // 2
    n_messages = n_fat + n_thin
    more = pltpu.SemaphoreType.DMA((n_messages,))
    state, marginal = pl.pallas_call(
        functools.partial(kernel, n_bank, n_lane, chunks),
        out_shape=(
            pltpu.VMEM(amplitudes.shape, f32),
            pltpu.VMEM(strip, f32),
        ),
        in_specs=[pl.BlockSpec(memory_space=pltpu.HBM)] * 3,
        out_specs=(whole, whole),
        scratch_shapes=[
            pltpu.VMEM(amplitudes.shape, f32),
            real,
            pltpu.VMEM(angles.shape, f32),
            pltpu.VMEM((TABLE, TABLE), jnp.bfloat16),
            pltpu.VMEM((blocks, 2, rows, lanes), f32),
            swapped, swapped, swapped, swapped,
            real, real, real,
            pltpu.VMEM((n_fat, n_bank, *part), f32),
            pltpu.VMEM((n_fat, n_bank - 1, *part), f32),
            pltpu.VMEM((max(n_thin, 1), n_bank, *thin), f32),
            pltpu.VMEM((max(n_thin, 1), n_bank - 1, *thin), f32),
            pltpu.SemaphoreType.DMA((3,)),
            pltpu.SemaphoreType.DMA((5,)),
            pltpu.SemaphoreType.DMA,
            pltpu.SemaphoreType.DMA((chunks,)),
            more, more,
            pltpu.SemaphoreType.REGULAR((4,)),
        ],
        compiler_params=pltpu.CompilerParams(
            collective_id=0, has_side_effects=True
        ),
        name="walsh",
    )(amplitudes, energies.reshape(devices, group, lanes), angles)
    return pl.pallas_call(
        put_out,
        out_shape=(
            jax.ShapeDtypeStruct(state.shape, f32),
            jax.ShapeDtypeStruct(marginal.shape, f32),
        ),
        in_specs=[whole] * 2,
        out_specs=(pl.BlockSpec(memory_space=pltpu.HBM),) * 2,
        scratch_shapes=[pltpu.SemaphoreType.DMA((2,))],
        compiler_params=pltpu.CompilerParams(vmem_limit_bytes=1024 * 1024),
        name="put_out",
    )(state, marginal)


def solution(mesh):
    sizes = mesh.shape
    return jax.shard_map(
        functools.partial(shards, sizes["bank"], sizes["lane"]),
        mesh=mesh,
        in_specs=(P(None, ("bank", "lane"), None, None), P(("bank", "lane"), None, None), P()),
        out_specs=(P(None, ("bank", "lane"), None, None), P("lane", "bank", None)),
        check_vma=False,
    )
```

```python
import functools

import jax
import jax.numpy as jnp
from jax import lax
from jax.experimental import pallas as pl
from jax.experimental.pallas import tpu as pltpu
from jax.sharding import PartitionSpec as P

MESH = pl.DeviceIdType.MESH
TABLE = 256
SUB = 8
HALF = SUB // 2
PLANES = 4


def walsh_table():
    both = lax.broadcasted_iota(jnp.int32, (TABLE, TABLE), 0)
    both = both & lax.broadcasted_iota(jnp.int32, (TABLE, TABLE), 1)
    for place in (4, 2, 1):
        both = both ^ (both >> place)
    sign = 1 - 2 * (both & 1)
    return (sign.astype(jnp.float32) * (1.0 / 16.0)).astype(jnp.bfloat16)


def cos_sin(turn):
    half = turn * 0.5
    x = half * half
    s = -1.0 / 39916800.0
    for term in (1.0 / 362880.0, -1.0 / 5040.0, 1.0 / 120.0, -1.0 / 6.0, 1.0):
        s = s * x + term
    s = s * half
    c = 1.0 / 479001600.0
    for term in (-1.0 / 3628800.0, 1.0 / 40320.0, -1.0 / 720.0, 1.0 / 24.0, -0.5, 1.0):
        c = c * x + term
    return 1.0 - 2.0 * (s * s), 2.0 * (s * c)


def split(values):
    high = values.astype(jnp.bfloat16)
    return high, (values - high.astype(jnp.float32)).astype(jnp.bfloat16)


def mix(items):
    items, step = list(items), 1
    while step < len(items):
        for low in range(len(items)):
            if not low & step:
                u, v = items[low], items[low + step]
                items[low], items[low + step] = u + v, u - v
        step *= 2
    return items


def dot(a, b):
    return jnp.dot(a, b, preferred_element_type=jnp.float32)


def mix_lanes(values, table):
    high, low = split(values)
    return dot(jnp.concatenate([high, low], axis=1), table[:, :128])


def kernel(
    n_bank, n_lane, chunks,
    a_hbm, e_hbm, angle_hbm,
    out_ref, marginal_ref,
    a_ref, e_ref, angle_ref, table_ref,
    held, sent1, got1, sent2, got2, levels, cosine, sine,
    chance, chances, thin_chance, thin_chances,
    in_sem, sent, e_recv, recv1, recv2, m_recv, known,
):
    devices = n_bank * n_lane
    _, blocks, rows, lanes = a_ref.shape
    group = blocks * rows // devices
    groups = rows // group
    bank, lane = lax.axis_index("bank"), lax.axis_index("lane")
    me = bank * n_lane + lane

    fetches = [
        pltpu.make_async_copy(src, dst, in_sem.at[i])
        for i, (src, dst) in enumerate([
            (e_hbm, e_ref), (a_hbm, a_ref), (angle_hbm, angle_ref),
        ])
    ]
    for fetch in fetches:
        fetch.start()

    deep = n_lane // PLANES
    lower = lane < n_lane // 2
    plane = lane // deep
    outer = (plane == 0) | (plane == PLANES - 1)

    def to_plane(far, act, start=0, count=deep):
        first = jnp.where(lower, PLANES - 1 - far, far) * deep + start

        def around(step, _):
            there = first + lax.rem(step + lane + 1, count)
            for turn in range(1, n_bank):
                act(lax.rem(bank + turn, n_bank), there)
            if far < PLANES // 2:
                act(bank, there)
            else:
                pl.when(there != lane)(lambda: act(bank, there))
            return 0

        lax.fori_loop(0, count, around, 0)

    def to_mirror(corner, act):
        first = (PLANES - 1 - plane) * deep
        pair = n_bank // 2
        opposite = lax.rem(bank // pair + 1, 2) * pair

        def around(step, _):
            there = first + lax.rem(step + lane, deep)
            for turn in range(pair):
                act(opposite + turn, there)
            return 0

        def beside(step, _):
            there = first + lax.rem(step + lane, deep)
            for turn in range(pair):
                act(bank // pair * pair + lax.rem(bank + turn, pair), there)
            return 0

        if corner:
            lax.fori_loop(1, deep, around, 0)
        else:
            lax.fori_loop(0, deep, beside, 0)
            around(0, 0)

    def others(act):
        for far in range(PLANES):
            to_plane(far, act)

    barrier = pltpu.get_barrier_semaphore()

    def greet(to_bank, to_lane):
        pl.semaphore_signal(
            barrier, inc=1, device_id=(to_bank, to_lane), device_id_type=MESH
        )

    next_lane = (plane + 1 - 2 * lax.rem(plane, 2)) * deep + lax.rem(lane, deep)
    mirror_lane = (PLANES - 1 - plane) * deep + lax.rem(lane, deep)

    def tell(step, to_lane):
        pl.semaphore_signal(
            known.at[step], inc=1, device_id=(bank, to_lane), device_id_type=MESH
        )

    @pl.when(outer)
    def _():
        greet(bank, next_lane)
        to_plane(3, greet)

    @pl.when(jnp.logical_not(outer))
    def _():
        to_plane(2, greet)
        to_mirror(False, greet)
        greet(bank, next_lane)

    table_ref[...] = walsh_table()
    fetches[0].wait()

    def give(src, dst, send_sem, recv_sem, to_bank, to_lane, spot=()):
        pltpu.make_async_remote_copy(
            src_ref=src.at[(to_bank * n_lane + to_lane, *spot)], dst_ref=dst.at[(me, *spot)],
            send_sem=send_sem, recv_sem=recv_sem,
            device_id=(to_bank, to_lane), device_id_type=MESH,
        ).start()

    def swap(*ends):
        others(functools.partial(give, *ends))

    def wait_for(buffer, sem):
        pltpu.make_async_copy(buffer, buffer, sem).wait()

    def arrive(buffer, sem, spot=()):
        wait_for(buffer.at[(pl.ds(0, devices - 1), *spot)], sem)

    give_e = functools.partial(give, e_ref, levels, sent.at[0], e_recv)

    @pl.when(outer)
    def _():
        pl.semaphore_wait(barrier, n_bank * deep)
        tell(0, next_lane)
        to_plane(3, give_e)
        pl.semaphore_wait(known.at[0], 1)
        to_plane(1, give_e)
        to_plane(2, give_e)
        pl.semaphore_wait(known.at[2], 1)
        to_plane(0, give_e)

    @pl.when(jnp.logical_not(outer))
    def _():
        pl.semaphore_wait(barrier, 2 * n_bank * deep - n_bank // 2 * (deep - 1))
        tell(3, mirror_lane)
        to_mirror(False, give_e)
        to_plane(2, give_e)
        pl.semaphore_wait(known.at[3], 1)
        tell(0, next_lane)
        to_mirror(True, give_e)
        pl.semaphore_wait(known.at[0], 1)
        tell(1, mirror_lane)
        to_plane(3, give_e)
        pl.semaphore_wait(known.at[1], 1)
        tell(2, next_lane)
        to_plane(0, give_e)

    levels[me] = e_ref[me]
    for fetch in fetches[1:]:
        fetch.wait()

    table = table_ref[...]

    def block_step(b, _):
        first = b * groups
        level = e_ref[pl.ds(first, groups)].reshape(rows, lanes)
        c, s = cos_sin(level * angle_ref[0:1, :])
        re, im = a_ref[0, b], a_ref[1, b]
        turned = jnp.concatenate([re * c + im * s, im * c - re * s], axis=0)
        along = mix_lanes(turned, table)
        high, low = split(jnp.concatenate([along[:rows], along[rows:]], axis=1))
        mixed = dot(table[:128, :], jnp.concatenate([high, low], axis=0))
        held[b, 0] = mixed[:, :lanes]
        held[b, 1] = mixed[:, lanes:]
        return 0

    lax.fori_loop(0, blocks, block_step, 0)

    for chunk in range(chunks):
        def spread(g, _, chunk=chunk):
            start = pl.multiple_of(g * group + chunk * SUB, SUB)
            for part in range(2):
                mixed = mix([held[b, part, pl.ds(start, SUB), :] for b in range(blocks)])
                for b in range(blocks):
                    sent1[chunk, b * groups + g, part] = mixed[b]
            return 0

        lax.fori_loop(0, groups, spread, 0)
        swap(sent1.at[chunk], got1.at[chunk], sent.at[1], recv1.at[chunk])
        got1[chunk, me] = sent1[chunk, me]

    arrive(levels, e_recv)

    def phases(d, _):
        c, s = cos_sin(levels[d] * angle_ref[1:2, :])
        cosine[d] = c
        sine[d] = s
        return 0

    lax.fori_loop(0, devices, phases, 0)

    wide = TABLE // SUB
    half = max(chunks // 2, 1)
    thin = (half - 1, chunks - 1) if half > 1 else ()
    fat = [c for c in range(chunks) if c not in thin]
    messages = [(c, ()) for c in fat] + [(c, (h,)) for c in thin for h in range(2)]
    few = blocks // 2

    def give_back(at, far, *some):
        chunk, spot = messages[at]
        ends = sent2.at[chunk], got2.at[chunk], sent.at[2], recv2.at[at]
        to_plane(far, lambda b, l: give(*ends, b, l, spot), *some)

    def send_back(order):
        for at, far, *some in order:
            give_back(at, far, *some)
        for at in sorted({at for at, *_ in order}):
            chunk, spot = messages[at]
            got2[(chunk, me, *spot)] = sent2[(chunk, me, *spot)]

    def far_first(*those):
        return [(at, far) for at in those for far in range(PLANES)]

    def take_back(at):
        chunk, spot = messages[at]
        arrive(got2.at[chunk], recv2.at[at], spot)

    for chunk in range(chunks):
        arrive(got1.at[chunk], recv1.at[chunk])
        if chunk == chunks - 1 > 0:
            pl.when(outer)(lambda: send_back(far_first(0)))
        there = pl.ds(chunk * SUB, SUB)
        re = mix([got1[chunk, d, 0] for d in range(devices)])
        im = mix([got1[chunk, d, 1] for d in range(devices)])
        done = []
        for start in range(0, devices, wide):
            r, i = [], []
            for d in range(start, start + wide):
                c, s = cosine[d, there, :], sine[d, there, :]
                r.append(re[d] * c + im[d] * s)
                i.append(im[d] * c - re[d] * s)
            along = mix_lanes(jnp.concatenate(r + i, axis=0), table)
            pair = jnp.concatenate([along[:TABLE], along[TABLE:]], axis=1)
            high, low = split(pair)
            done.append(dot(table, high) + dot(table, low))
        done = mix(done)
        first = chunk - chunk % half
        last = chunk % half == half - 1
        for d in range(devices):
            at = d % wide * SUB
            for part in range(2):
                tile = done[d // wide][at : at + SUB, part * lanes : (part + 1) * lanes]
                if last:
                    tiles = mix([sent2[c, d, part] for c in range(first, chunk)] + [tile])
                    for c in range(half):
                        sent2[first + c, d, part] = tiles[c]
                else:
                    sent2[chunk, d, part] = tile
        if last and first == chunk + 1 - chunks:
            send_back(far_first(0))
        elif last and first == 0:
            pl.when(jnp.logical_not(outer))(lambda: send_back(far_first(0)))
        elif last:
            send_back(far_first(fat.index(first)))

    for chunk in range(1, half):
        def halves(d, _, chunk=chunk):
            u, v = sent2[chunk, d], sent2[chunk + half, d]
            for to, both in ((chunk, u + v), (chunk + half, u - v)):
                if to in thin:
                    both = [
                        jnp.concatenate([part[h * HALF : (h + 1) * HALF] for part in both])
                        for h in range(2)
                    ]
                for i in range(2):
                    sent2[to, d, i] = both[i]
            return 0

        lax.fori_loop(0, devices, halves, 0)

    scale = float(TABLE * TABLE) / (devices * blocks * rows * lanes)
    share = rows // n_bank // group
    slim = list(range(len(fat), len(messages)))
    steps = [(0, fat.index(half))] if chunks > 1 else [(0,)]
    for first in range(1, half - 1):
        steps += [(fat.index(c),) for c in (first, first + half)]
        send_back(far_first(*steps[-2], *steps[-1]))
    steps += [(at,) for at in slim]
    rows_of = [(far, start, deep // 2) for far in (0, 1) for start in (0, deep // 2)]
    order = [(0, 0), (1, 0), (2, 0), (3, 0), (0, 1), (1, 1), (0, 2), (0, 3), (2, 1), (1, 2), (1, 3), (3, 1), (2, 2), (2, 3), (3, 2), (3, 3)]
    send_back([(at, far) for at in slim for far in (2, 3)])
    if slim:
        send_back([(slim[i], *rows_of[j]) for i, j in order])

    def back(chunk, part):
        return mix([got2[chunk, d, part] for d in range(devices)])

    def whole(step):
        places = [messages[at][0] for at in step]
        for at, chunk in zip(step[:-1], places):
            take_back(at)
            for part in range(2):
                mixed = back(chunk, part)
                for d in range(devices):
                    got2[chunk, d, part] = mixed[d]
        take_back(step[-1])
        for part in range(2):
            mixed = back(places[-1], part)
            for d in range(devices):
                tiles = mix([got2[c, d, part] for c in places[:-1]] + [mixed[d]])
                b, g = divmod(d, groups)
                for at, chunk, tile in zip(step, places, tiles):
                    value = tile * scale
                    row = g * group + chunk * SUB
                    out_ref[part, b, row : row + SUB, :] = value
                    spot = (at, g // share, b, pl.ds(g % share * SUB, SUB))
                    square = value * value
                    chance[spot] = chance[spot] + square if part else square

    def thinner(at):
        take_back(at)
        chunk, (h,) = messages[at]
        mixed = back(chunk, h)
        for d in range(devices):
            b, g = divmod(d, groups)
            value = mixed[d] * scale
            row = g * group + chunk * SUB + h * HALF
            for part in range(2):
                out_ref[part, b, row : row + HALF, :] = value[part * HALF : (part + 1) * HALF]
            square = value * value
            low, high = b % few, b // few
            spot = (at - len(fat), g // share, low, pl.ds(g % share * SUB + high * HALF, HALF))
            thin_chance[spot] = square[:HALF] + square[HALF:]

    for step in steps:
        if step[0] < len(fat):
            whole(step)
        else:
            thinner(step[0])
        for at in step:
            src, dst, place, group_sem = chance, chances, at, 3
            if at >= len(fat):
                src, dst, place, group_sem = thin_chance, thin_chances, at - len(fat), 4
            for turn in range(1, n_bank):
                other = lax.rem(bank + turn, n_bank)
                pltpu.make_async_remote_copy(
                    src_ref=src.at[place, other], dst_ref=dst.at[place, turn - 1],
                    send_sem=sent.at[group_sem], recv_sem=m_recv.at[at],
                    device_id=(other, lane), device_id_type=MESH,
                ).start()
    for step in steps:
        for at in step:
            src, dst, place = chance, chances, at
            if at >= len(fat):
                src, dst, place = thin_chance, thin_chances, at - len(fat)
            wait_for(dst.at[place], m_recv.at[at])
            total = src[place, bank]
            for turn in range(1, n_bank):
                total = total + dst[place, turn - 1]
            total = total * (1.0 / n_bank)
            chunk, spot = messages[at]
            for g in range(share):
                row = g * group + chunk * SUB
                if not spot:
                    marginal_ref[:, row : row + SUB, :] = total[:, g * SUB : (g + 1) * SUB]
                    continue
                row = row + spot[0] * HALF
                for high in range(2):
                    at_row = g * SUB + high * HALF
                    marginal_ref[high * few : (high + 1) * few, row : row + HALF, :] = (
                        total[:, at_row : at_row + HALF]
                    )

    wait_for(chances, sent.at[3])
    if slim:
        wait_for(thin_chances, sent.at[4])
    arrive(e_ref, sent.at[0])
    wait_for(sent1.at[:, pl.ds(0, devices - 1)], sent.at[1])
    wait_for(sent2.at[:, pl.ds(0, devices - 1)], sent.at[2])


def put_out(state_ref, marginal_ref, state_out, marginal_out, sem):
    copies = [
        pltpu.make_async_copy(state_ref, state_out, sem.at[0]),
        pltpu.make_async_copy(marginal_ref, marginal_out, sem.at[1]),
    ]
    for copy in copies:
        copy.start()
    for copy in copies:
        copy.wait()


def shards(n_bank, n_lane, amplitudes, energies, angles):
    devices = n_bank * n_lane
    _, blocks, rows, lanes = amplitudes.shape
    group = blocks * rows // devices
    chunks = group // SUB
    f32 = jnp.float32
    whole = pl.BlockSpec(memory_space=pltpu.VMEM)
    swapped = pltpu.VMEM((chunks, devices, 2, SUB, lanes), f32)
    real = pltpu.VMEM((devices, group, lanes), f32)
    strip = (blocks, rows // n_bank, lanes)
    part = (blocks, rows // n_bank // chunks, lanes)
    thin = (blocks // 2, rows // n_bank // chunks, lanes)
    n_thin = 4 if chunks > 2 else 0
    n_fat = chunks - n_thin // 2
    n_messages = n_fat + n_thin
    more = pltpu.SemaphoreType.DMA((n_messages,))
    state, marginal = pl.pallas_call(
        functools.partial(kernel, n_bank, n_lane, chunks),
        out_shape=(
            pltpu.VMEM(amplitudes.shape, f32),
            pltpu.VMEM(strip, f32),
        ),
        in_specs=[pl.BlockSpec(memory_space=pltpu.HBM)] * 3,
        out_specs=(whole, whole),
        scratch_shapes=[
            pltpu.VMEM(amplitudes.shape, f32),
            real,
            pltpu.VMEM(angles.shape, f32),
            pltpu.VMEM((TABLE, TABLE), jnp.bfloat16),
            pltpu.VMEM((blocks, 2, rows, lanes), f32),
            swapped, swapped, swapped, swapped,
            real, real, real,
            pltpu.VMEM((n_fat, n_bank, *part), f32),
            pltpu.VMEM((n_fat, n_bank - 1, *part), f32),
            pltpu.VMEM((max(n_thin, 1), n_bank, *thin), f32),
            pltpu.VMEM((max(n_thin, 1), n_bank - 1, *thin), f32),
            pltpu.SemaphoreType.DMA((3,)),
            pltpu.SemaphoreType.DMA((5,)),
            pltpu.SemaphoreType.DMA,
            pltpu.SemaphoreType.DMA((chunks,)),
            more, more,
            pltpu.SemaphoreType.REGULAR((4,)),
        ],
        compiler_params=pltpu.CompilerParams(
            collective_id=0, has_side_effects=True
        ),
        name="walsh",
    )(amplitudes, energies.reshape(devices, group, lanes), angles)
    return pl.pallas_call(
        put_out,
        out_shape=(
            jax.ShapeDtypeStruct(state.shape, f32),
            jax.ShapeDtypeStruct(marginal.shape, f32),
        ),
        in_specs=[whole] * 2,
        out_specs=(pl.BlockSpec(memory_space=pltpu.HBM),) * 2,
        scratch_shapes=[pltpu.SemaphoreType.DMA((2,))],
        compiler_params=pltpu.CompilerParams(vmem_limit_bytes=1024 * 1024),
        name="put_out",
    )(state, marginal)


def solution(mesh):
    sizes = mesh.shape
    return jax.shard_map(
        functools.partial(shards, sizes["bank"], sizes["lane"]),
        mesh=mesh,
        in_specs=(P(None, ("bank", "lane"), None, None), P(("bank", "lane"), None, None), P()),
        out_specs=(P(None, ("bank", "lane"), None, None), P("lane", "bank", None)),
        check_vma=False,
    )
```

```python
import functools

import jax
import jax.numpy as jnp
from jax import lax
from jax.experimental import pallas as pl
from jax.experimental.pallas import tpu as pltpu
from jax.sharding import PartitionSpec as P

MESH = pl.DeviceIdType.MESH
TABLE = 256
SUB = 8
HALF = SUB // 2
PLANES = 4


def walsh_table():
    both = lax.broadcasted_iota(jnp.int32, (TABLE, TABLE), 0)
    both = both & lax.broadcasted_iota(jnp.int32, (TABLE, TABLE), 1)
    for place in (4, 2, 1):
        both = both ^ (both >> place)
    sign = 1 - 2 * (both & 1)
    return (sign.astype(jnp.float32) * (1.0 / 16.0)).astype(jnp.bfloat16)


def cos_sin(turn):
    half = turn * 0.5
    x = half * half
    s = -1.0 / 39916800.0
    for term in (1.0 / 362880.0, -1.0 / 5040.0, 1.0 / 120.0, -1.0 / 6.0, 1.0):
        s = s * x + term
    s = s * half
    c = 1.0 / 479001600.0
    for term in (-1.0 / 3628800.0, 1.0 / 40320.0, -1.0 / 720.0, 1.0 / 24.0, -0.5, 1.0):
        c = c * x + term
    return 1.0 - 2.0 * (s * s), 2.0 * (s * c)


def split(values):
    high = values.astype(jnp.bfloat16)
    return high, (values - high.astype(jnp.float32)).astype(jnp.bfloat16)


def mix(items):
    items, step = list(items), 1
    while step < len(items):
        for low in range(len(items)):
            if not low & step:
                u, v = items[low], items[low + step]
                items[low], items[low + step] = u + v, u - v
        step *= 2
    return items


def dot(a, b):
    return jnp.dot(a, b, preferred_element_type=jnp.float32)


def mix_lanes(values, table):
    high, low = split(values)
    return dot(jnp.concatenate([high, low], axis=1), table[:, :128])


def kernel(
    n_bank, n_lane, chunks,
    a_hbm, e_hbm, angle_hbm,
    out_ref, marginal_ref,
    a_ref, e_ref, angle_ref, table_ref,
    held, sent1, got1, sent2, got2, levels, cosine, sine,
    chance, chances, thin_chance, thin_chances,
    in_sem, sent, e_recv, recv1, recv2, m_recv, known,
):
    devices = n_bank * n_lane
    _, blocks, rows, lanes = a_ref.shape
    group = blocks * rows // devices
    groups = rows // group
    bank, lane = lax.axis_index("bank"), lax.axis_index("lane")
    me = bank * n_lane + lane

    fetches = [
        pltpu.make_async_copy(src, dst, in_sem.at[i])
        for i, (src, dst) in enumerate([
            (e_hbm, e_ref), (a_hbm, a_ref), (angle_hbm, angle_ref),
        ])
    ]
    deep = n_lane // PLANES
    lower = lane < n_lane // 2
    plane = lane // deep
    outer = (plane == 0) | (plane == PLANES - 1)

    def to_plane(far, act, start=0, count=deep):
        first = jnp.where(lower, PLANES - 1 - far, far) * deep + start

        def around(step, _):
            there = first + lax.rem(step + lane + 1, count)
            for turn in range(1, n_bank):
                act(lax.rem(bank + turn, n_bank), there)
            if far < PLANES // 2:
                act(bank, there)
            else:
                pl.when(there != lane)(lambda: act(bank, there))
            return 0

        lax.fori_loop(0, count, around, 0)

    def to_mirror(corner, act):
        first = (PLANES - 1 - plane) * deep
        pair = n_bank // 2
        opposite = lax.rem(bank // pair + 1, 2) * pair

        def around(step, _):
            there = first + lax.rem(step + lane, deep)
            for turn in range(pair):
                act(opposite + turn, there)
            return 0

        def beside(step, _):
            there = first + lax.rem(step + lane, deep)
            for turn in range(pair):
                act(bank // pair * pair + lax.rem(bank + turn, pair), there)
            return 0

        if corner:
            lax.fori_loop(1, deep, around, 0)
        else:
            lax.fori_loop(0, deep, beside, 0)
            around(0, 0)

    def others(act):
        for far in range(PLANES):
            to_plane(far, act)

    barrier = pltpu.get_barrier_semaphore()

    def greet(to_bank, to_lane):
        pl.semaphore_signal(
            barrier, inc=1, device_id=(to_bank, to_lane), device_id_type=MESH
        )

    next_lane = (plane + 1 - 2 * lax.rem(plane, 2)) * deep + lax.rem(lane, deep)
    mirror_lane = (PLANES - 1 - plane) * deep + lax.rem(lane, deep)

    def tell(step, to_lane):
        pl.semaphore_signal(
            known.at[step], inc=1, device_id=(bank, to_lane), device_id_type=MESH
        )

    @pl.when(outer)
    def _():
        greet(bank, next_lane)
        to_plane(3, greet)

    @pl.when(jnp.logical_not(outer))
    def _():
        to_mirror(False, greet)
        greet(bank, next_lane)
        to_plane(2, greet)

    for fetch in fetches:
        fetch.start()
    table_ref[...] = walsh_table()
    fetches[0].wait()

    def give(src, dst, send_sem, recv_sem, to_bank, to_lane, spot=()):
        pltpu.make_async_remote_copy(
            src_ref=src.at[(to_bank * n_lane + to_lane, *spot)], dst_ref=dst.at[(me, *spot)],
            send_sem=send_sem, recv_sem=recv_sem,
            device_id=(to_bank, to_lane), device_id_type=MESH,
        ).start()

    def swap(*ends):
        others(functools.partial(give, *ends))

    def wait_for(buffer, sem):
        pltpu.make_async_copy(buffer, buffer, sem).wait()

    def arrive(buffer, sem, spot=()):
        wait_for(buffer.at[(pl.ds(0, devices - 1), *spot)], sem)

    give_e = functools.partial(give, e_ref, levels, sent.at[0], e_recv)

    @pl.when(outer)
    def _():
        pl.semaphore_wait(barrier, n_bank * deep)
        tell(0, next_lane)
        to_plane(3, give_e)
        pl.semaphore_wait(known.at[0], 1)
        to_plane(1, give_e)
        to_plane(2, give_e)
        pl.semaphore_wait(known.at[2], 1)
        to_plane(0, give_e)

    @pl.when(jnp.logical_not(outer))
    def _():
        pl.semaphore_wait(barrier, 2 * n_bank * deep - n_bank // 2 * (deep - 1))
        tell(3, mirror_lane)
        to_mirror(False, give_e)
        to_plane(2, give_e)
        pl.semaphore_wait(known.at[3], 1)
        tell(0, next_lane)
        to_mirror(True, give_e)
        pl.semaphore_wait(known.at[0], 1)
        tell(1, mirror_lane)
        to_plane(3, give_e)
        pl.semaphore_wait(known.at[1], 1)
        tell(2, next_lane)
        to_plane(0, give_e)

    levels[me] = e_ref[me]
    for fetch in fetches[1:]:
        fetch.wait()

    table = table_ref[...]

    def block_step(b, _):
        first = b * groups
        level = e_ref[pl.ds(first, groups)].reshape(rows, lanes)
        c, s = cos_sin(level * angle_ref[0:1, :])
        re, im = a_ref[0, b], a_ref[1, b]
        turned = jnp.concatenate([re * c + im * s, im * c - re * s], axis=0)
        along = mix_lanes(turned, table)
        high, low = split(jnp.concatenate([along[:rows], along[rows:]], axis=1))
        mixed = dot(table[:128, :], jnp.concatenate([high, low], axis=0))
        held[b, 0] = mixed[:, :lanes]
        held[b, 1] = mixed[:, lanes:]
        return 0

    lax.fori_loop(0, blocks, block_step, 0)

    for chunk in range(chunks):
        def spread(g, _, chunk=chunk):
            start = pl.multiple_of(g * group + chunk * SUB, SUB)
            for part in range(2):
                mixed = mix([held[b, part, pl.ds(start, SUB), :] for b in range(blocks)])
                for b in range(blocks):
                    sent1[chunk, b * groups + g, part] = mixed[b]
            return 0

        lax.fori_loop(0, groups, spread, 0)
        swap(sent1.at[chunk], got1.at[chunk], sent.at[1], recv1.at[chunk])
        got1[chunk, me] = sent1[chunk, me]

    arrive(levels, e_recv)

    def phases(d, _):
        c, s = cos_sin(levels[d] * angle_ref[1:2, :])
        cosine[d] = c
        sine[d] = s
        return 0

    lax.fori_loop(0, devices, phases, 0)

    wide = TABLE // SUB
    half = max(chunks // 2, 1)
    thin = (half - 1, chunks - 1) if half > 1 else ()
    fat = [c for c in range(chunks) if c not in thin]
    messages = [(c, ()) for c in fat] + [(c, (h,)) for c in thin for h in range(2)]
    few = blocks // 2

    def give_back(at, far, *some):
        chunk, spot = messages[at]
        ends = sent2.at[chunk], got2.at[chunk], sent.at[2], recv2.at[at]
        to_plane(far, lambda b, l: give(*ends, b, l, spot), *some)

    def send_back(order):
        for at, far, *some in order:
            give_back(at, far, *some)
        for at in sorted({at for at, *_ in order}):
            chunk, spot = messages[at]
            got2[(chunk, me, *spot)] = sent2[(chunk, me, *spot)]

    def far_first(*those):
        return [(at, far) for at in those for far in range(PLANES)]

    def take_back(at):
        chunk, spot = messages[at]
        arrive(got2.at[chunk], recv2.at[at], spot)

    for chunk in range(chunks):
        arrive(got1.at[chunk], recv1.at[chunk])
        if chunk == chunks - 1 > 0:
            pl.when(outer)(lambda: send_back(far_first(0)))
        there = pl.ds(chunk * SUB, SUB)
        re = mix([got1[chunk, d, 0] for d in range(devices)])
        im = mix([got1[chunk, d, 1] for d in range(devices)])
        done = []
        for start in range(0, devices, wide):
            r, i = [], []
            for d in range(start, start + wide):
                c, s = cosine[d, there, :], sine[d, there, :]
                r.append(re[d] * c + im[d] * s)
                i.append(im[d] * c - re[d] * s)
            along = mix_lanes(jnp.concatenate(r + i, axis=0), table)
            pair = jnp.concatenate([along[:TABLE], along[TABLE:]], axis=1)
            high, low = split(pair)
            done.append(dot(table, high) + dot(table, low))
        done = mix(done)
        first = chunk - chunk % half
        last = chunk % half == half - 1
        for d in range(devices):
            at = d % wide * SUB
            for part in range(2):
                tile = done[d // wide][at : at + SUB, part * lanes : (part + 1) * lanes]
                if last:
                    tiles = mix([sent2[c, d, part] for c in range(first, chunk)] + [tile])
                    for c in range(half):
                        sent2[first + c, d, part] = tiles[c]
                else:
                    sent2[chunk, d, part] = tile
        if last and first == chunk + 1 - chunks:
            send_back(far_first(0))
        elif last and first == 0:
            pl.when(jnp.logical_not(outer))(lambda: send_back(far_first(0)))
        elif last:
            send_back(far_first(fat.index(first)))

    for chunk in range(1, half):
        def halves(d, _, chunk=chunk):
            u, v = sent2[chunk, d], sent2[chunk + half, d]
            for to, both in ((chunk, u + v), (chunk + half, u - v)):
                if to in thin:
                    both = [
                        jnp.concatenate([part[h * HALF : (h + 1) * HALF] for part in both])
                        for h in range(2)
                    ]
                for i in range(2):
                    sent2[to, d, i] = both[i]
            return 0

        lax.fori_loop(0, devices, halves, 0)

    scale = float(TABLE * TABLE) / (devices * blocks * rows * lanes)
    share = rows // n_bank // group
    slim = list(range(len(fat), len(messages)))
    steps = [(0, fat.index(half))] if chunks > 1 else [(0,)]
    for first in range(1, half - 1):
        steps += [(fat.index(c),) for c in (first, first + half)]
        send_back(far_first(*steps[-2], *steps[-1]))
    steps += [(at,) for at in slim]
    rows_of = [(far, start, deep // 2) for far in (0, 1) for start in (0, deep // 2)]
    order = [(0, 0), (1, 0), (2, 0), (3, 0), (0, 1), (1, 1), (0, 2), (0, 3), (2, 1), (1, 2), (1, 3), (3, 1), (2, 2), (2, 3), (3, 2), (3, 3)]
    send_back([(at, far) for at in slim for far in (2, 3)])
    if slim:
        send_back([(slim[i], *rows_of[j]) for i, j in order])

    def back(chunk, part):
        return mix([got2[chunk, d, part] for d in range(devices)])

    def whole(step):
        places = [messages[at][0] for at in step]
        for at, chunk in zip(step[:-1], places):
            take_back(at)
            for part in range(2):
                mixed = back(chunk, part)
                for d in range(devices):
                    got2[chunk, d, part] = mixed[d]
        take_back(step[-1])
        for part in range(2):
            mixed = back(places[-1], part)
            for d in range(devices):
                tiles = mix([got2[c, d, part] for c in places[:-1]] + [mixed[d]])
                b, g = divmod(d, groups)
                for at, chunk, tile in zip(step, places, tiles):
                    value = tile * scale
                    row = g * group + chunk * SUB
                    out_ref[part, b, row : row + SUB, :] = value
                    spot = (at, g // share, b, pl.ds(g % share * SUB, SUB))
                    square = value * value
                    chance[spot] = chance[spot] + square if part else square

    def thinner(at):
        take_back(at)
        chunk, (h,) = messages[at]
        mixed = back(chunk, h)
        for d in range(devices):
            b, g = divmod(d, groups)
            value = mixed[d] * scale
            row = g * group + chunk * SUB + h * HALF
            for part in range(2):
                out_ref[part, b, row : row + HALF, :] = value[part * HALF : (part + 1) * HALF]
            square = value * value
            low, high = b % few, b // few
            spot = (at - len(fat), g // share, low, pl.ds(g % share * SUB + high * HALF, HALF))
            thin_chance[spot] = square[:HALF] + square[HALF:]

    for step in steps:
        if step[0] < len(fat):
            whole(step)
        else:
            thinner(step[0])
        for at in step:
            src, dst, place, group_sem = chance, chances, at, 3
            if at >= len(fat):
                src, dst, place, group_sem = thin_chance, thin_chances, at - len(fat), 4
            for turn in range(1, n_bank):
                other = lax.rem(bank + turn, n_bank)
                pltpu.make_async_remote_copy(
                    src_ref=src.at[place, other], dst_ref=dst.at[place, turn - 1],
                    send_sem=sent.at[group_sem], recv_sem=m_recv.at[group_sem - 3],
                    device_id=(other, lane), device_id_type=MESH,
                ).start()
    wait_for(chances, m_recv.at[0])
    if slim:
        wait_for(thin_chances, m_recv.at[1])
    for step in steps:
        for at in step:
            src, dst, place = chance, chances, at
            if at >= len(fat):
                src, dst, place = thin_chance, thin_chances, at - len(fat)
            total = src[place, bank]
            for turn in range(1, n_bank):
                total = total + dst[place, turn - 1]
            total = total * (1.0 / n_bank)
            chunk, spot = messages[at]
            for g in range(share):
                row = g * group + chunk * SUB
                if not spot:
                    marginal_ref[:, row : row + SUB, :] = total[:, g * SUB : (g + 1) * SUB]
                    continue
                row = row + spot[0] * HALF
                for high in range(2):
                    at_row = g * SUB + high * HALF
                    marginal_ref[high * few : (high + 1) * few, row : row + HALF, :] = (
                        total[:, at_row : at_row + HALF]
                    )

    wait_for(chances, sent.at[3])
    if slim:
        wait_for(thin_chances, sent.at[4])
    arrive(e_ref, sent.at[0])
    wait_for(sent1.at[:, pl.ds(0, devices - 1)], sent.at[1])
    wait_for(sent2.at[:, pl.ds(0, devices - 1)], sent.at[2])


def put_out(state_ref, marginal_ref, state_out, marginal_out, sem):
    copies = [
        pltpu.make_async_copy(state_ref, state_out, sem.at[0]),
        pltpu.make_async_copy(marginal_ref, marginal_out, sem.at[1]),
    ]
    for copy in copies:
        copy.start()
    for copy in copies:
        copy.wait()


def shards(n_bank, n_lane, amplitudes, energies, angles):
    devices = n_bank * n_lane
    _, blocks, rows, lanes = amplitudes.shape
    group = blocks * rows // devices
    chunks = group // SUB
    f32 = jnp.float32
    whole = pl.BlockSpec(memory_space=pltpu.VMEM)
    swapped = pltpu.VMEM((chunks, devices, 2, SUB, lanes), f32)
    real = pltpu.VMEM((devices, group, lanes), f32)
    strip = (blocks, rows // n_bank, lanes)
    part = (blocks, rows // n_bank // chunks, lanes)
    thin = (blocks // 2, rows // n_bank // chunks, lanes)
    n_thin = 4 if chunks > 2 else 0
    n_fat = chunks - n_thin // 2
    n_messages = n_fat + n_thin
    more = pltpu.SemaphoreType.DMA((n_messages,))
    state, marginal = pl.pallas_call(
        functools.partial(kernel, n_bank, n_lane, chunks),
        out_shape=(
            pltpu.VMEM(amplitudes.shape, f32),
            pltpu.VMEM(strip, f32),
        ),
        in_specs=[pl.BlockSpec(memory_space=pltpu.HBM)] * 3,
        out_specs=(whole, whole),
        scratch_shapes=[
            pltpu.VMEM(amplitudes.shape, f32),
            real,
            pltpu.VMEM(angles.shape, f32),
            pltpu.VMEM((TABLE, TABLE), jnp.bfloat16),
            pltpu.VMEM((blocks, 2, rows, lanes), f32),
            swapped, swapped, swapped, swapped,
            real, real, real,
            pltpu.VMEM((n_fat, n_bank, *part), f32),
            pltpu.VMEM((n_fat, n_bank - 1, *part), f32),
            pltpu.VMEM((max(n_thin, 1), n_bank, *thin), f32),
            pltpu.VMEM((max(n_thin, 1), n_bank - 1, *thin), f32),
            pltpu.SemaphoreType.DMA((3,)),
            pltpu.SemaphoreType.DMA((5,)),
            pltpu.SemaphoreType.DMA,
            pltpu.SemaphoreType.DMA((chunks,)),
            more,
            pltpu.SemaphoreType.DMA((2,)),
            pltpu.SemaphoreType.REGULAR((4,)),
        ],
        compiler_params=pltpu.CompilerParams(
            collective_id=0, has_side_effects=True
        ),
        name="walsh",
    )(amplitudes, energies.reshape(devices, group, lanes), angles)
    return pl.pallas_call(
        put_out,
        out_shape=(
            jax.ShapeDtypeStruct(state.shape, f32),
            jax.ShapeDtypeStruct(marginal.shape, f32),
        ),
        in_specs=[whole] * 2,
        out_specs=(pl.BlockSpec(memory_space=pltpu.HBM),) * 2,
        scratch_shapes=[pltpu.SemaphoreType.DMA((2,))],
        compiler_params=pltpu.CompilerParams(vmem_limit_bytes=1024 * 1024),
        name="put_out",
    )(state, marginal)


def solution(mesh):
    sizes = mesh.shape
    return jax.shard_map(
        functools.partial(shards, sizes["bank"], sizes["lane"]),
        mesh=mesh,
        in_specs=(P(None, ("bank", "lane"), None, None), P(("bank", "lane"), None, None), P()),
        out_specs=(P(None, ("bank", "lane"), None, None), P("lane", "bank", None)),
        check_vma=False,
    )
```

```python
import functools

import jax
import jax.numpy as jnp
from jax import lax
from jax.experimental import pallas as pl
from jax.experimental.pallas import tpu as pltpu
from jax.sharding import PartitionSpec as P

MESH = pl.DeviceIdType.MESH
TABLE = 256
SUB = 8
HALF = SUB // 2
PLANES = 4


def walsh_table():
    both = lax.broadcasted_iota(jnp.int32, (TABLE, TABLE), 0)
    both = both & lax.broadcasted_iota(jnp.int32, (TABLE, TABLE), 1)
    for place in (4, 2, 1):
        both = both ^ (both >> place)
    sign = 1 - 2 * (both & 1)
    return (sign.astype(jnp.float32) * (1.0 / 16.0)).astype(jnp.bfloat16)


def cos_sin(turn):
    half = turn * 0.5
    x = half * half
    s = -1.0 / 39916800.0
    for term in (1.0 / 362880.0, -1.0 / 5040.0, 1.0 / 120.0, -1.0 / 6.0, 1.0):
        s = s * x + term
    s = s * half
    c = 1.0 / 479001600.0
    for term in (-1.0 / 3628800.0, 1.0 / 40320.0, -1.0 / 720.0, 1.0 / 24.0, -0.5, 1.0):
        c = c * x + term
    return 1.0 - 2.0 * (s * s), 2.0 * (s * c)


def split(values):
    high = values.astype(jnp.bfloat16)
    return high, (values - high.astype(jnp.float32)).astype(jnp.bfloat16)


def mix(items):
    items, step = list(items), 1
    while step < len(items):
        for low in range(len(items)):
            if not low & step:
                u, v = items[low], items[low + step]
                items[low], items[low + step] = u + v, u - v
        step *= 2
    return items


def dot(a, b):
    return jnp.dot(a, b, preferred_element_type=jnp.float32)


def mix_lanes(values, table):
    high, low = split(values)
    return dot(jnp.concatenate([high, low], axis=1), table[:, :128])


def kernel(
    n_bank, n_lane, chunks,
    a_hbm, e_hbm, angle_hbm,
    out_ref, marginal_ref,
    a_ref, e_ref, angle_ref, table_ref,
    held, sent1, got1, sent2, got2, levels, cosine, sine,
    chance, chances, thin_chance, thin_chances,
    in_sem, sent, e_recv, recv1, recv2, m_recv, known,
):
    devices = n_bank * n_lane
    _, blocks, rows, lanes = a_ref.shape
    group = blocks * rows // devices
    groups = rows // group
    bank, lane = lax.axis_index("bank"), lax.axis_index("lane")
    me = bank * n_lane + lane

    fetches = [
        pltpu.make_async_copy(src, dst, in_sem.at[i])
        for i, (src, dst) in enumerate([
            (e_hbm, e_ref), (a_hbm, a_ref), (angle_hbm, angle_ref),
        ])
    ]
    deep = n_lane // PLANES
    lower = lane < n_lane // 2
    plane = lane // deep
    outer = (plane == 0) | (plane == PLANES - 1)

    def to_plane(far, act, start=0, count=deep):
        first = jnp.where(lower, PLANES - 1 - far, far) * deep + start

        def around(step, _):
            there = first + lax.rem(step + lane + 1, count)
            for turn in range(1, n_bank):
                act(lax.rem(bank + turn, n_bank), there)
            if far < PLANES // 2:
                act(bank, there)
            else:
                pl.when(there != lane)(lambda: act(bank, there))
            return 0

        lax.fori_loop(0, count, around, 0)

    def to_mirror(corner, act):
        first = (PLANES - 1 - plane) * deep
        pair = n_bank // 2
        opposite = lax.rem(bank // pair + 1, 2) * pair

        def around(step, _):
            there = first + lax.rem(step + lane, deep)
            for turn in range(pair):
                act(opposite + turn, there)
            return 0

        def beside(step, _):
            there = first + lax.rem(step + lane, deep)
            for turn in range(pair):
                act(bank // pair * pair + lax.rem(bank + turn, pair), there)
            return 0

        if corner:
            lax.fori_loop(1, deep, around, 0)
        else:
            lax.fori_loop(0, deep, beside, 0)
            around(0, 0)

    def others(act):
        for far in range(PLANES):
            to_plane(far, act)

    barrier = pltpu.get_barrier_semaphore()

    def greet(to_bank, to_lane):
        pl.semaphore_signal(
            barrier, inc=1, device_id=(to_bank, to_lane), device_id_type=MESH
        )

    next_lane = (plane + 1 - 2 * lax.rem(plane, 2)) * deep + lax.rem(lane, deep)
    mirror_lane = (PLANES - 1 - plane) * deep + lax.rem(lane, deep)

    def tell(step, to_lane):
        pl.semaphore_signal(
            known.at[step], inc=1, device_id=(bank, to_lane), device_id_type=MESH
        )

    @pl.when(outer)
    def _():
        greet(bank, next_lane)
        to_plane(3, greet)

    @pl.when(jnp.logical_not(outer))
    def _():
        to_mirror(False, greet)
        greet(bank, next_lane)
        to_plane(2, greet)

    for fetch in fetches:
        fetch.start()
    table_ref[...] = walsh_table()
    fetches[0].wait()

    def give(src, dst, send_sem, recv_sem, to_bank, to_lane, spot=()):
        pltpu.make_async_remote_copy(
            src_ref=src.at[(to_bank * n_lane + to_lane, *spot)], dst_ref=dst.at[(me, *spot)],
            send_sem=send_sem, recv_sem=recv_sem,
            device_id=(to_bank, to_lane), device_id_type=MESH,
        ).start()

    def swap(*ends):
        others(functools.partial(give, *ends))

    def wait_for(buffer, sem):
        pltpu.make_async_copy(buffer, buffer, sem).wait()

    def arrive(buffer, sem, spot=()):
        wait_for(buffer.at[(pl.ds(0, devices - 1), *spot)], sem)

    give_e = functools.partial(give, e_ref, levels, sent.at[0], e_recv)

    @pl.when(outer)
    def _():
        pl.semaphore_wait(barrier, n_bank * deep)
        tell(0, next_lane)
        to_plane(3, give_e)
        pl.semaphore_wait(known.at[0], 1)
        to_plane(1, give_e)
        to_plane(2, give_e)

    @pl.when(jnp.logical_not(outer))
    def _():
        pl.semaphore_wait(barrier, 2 * n_bank * deep - n_bank // 2 * (deep - 1))
        tell(3, mirror_lane)
        to_mirror(False, give_e)
        to_plane(2, give_e)
        pl.semaphore_wait(known.at[3], 1)
        tell(0, next_lane)
        to_mirror(True, give_e)
        pl.semaphore_wait(known.at[0], 1)
        tell(1, mirror_lane)
        to_plane(3, give_e)

    levels[me] = e_ref[me]
    for fetch in fetches[1:]:
        fetch.wait()

    table = table_ref[...]

    def block_step(b, _):
        first = b * groups
        level = e_ref[pl.ds(first, groups)].reshape(rows, lanes)
        c, s = cos_sin(level * angle_ref[0:1, :])
        re, im = a_ref[0, b], a_ref[1, b]
        turned = jnp.concatenate([re * c + im * s, im * c - re * s], axis=0)
        along = mix_lanes(turned, table)
        high, low = split(jnp.concatenate([along[:rows], along[rows:]], axis=1))
        mixed = dot(table[:128, :], jnp.concatenate([high, low], axis=0))
        held[b, 0] = mixed[:, :lanes]
        held[b, 1] = mixed[:, lanes:]
        return 0

    lax.fori_loop(0, blocks, block_step, 0)

    @pl.when(outer)
    def _():
        pl.semaphore_wait(known.at[2], 1)
        to_plane(0, give_e)

    @pl.when(jnp.logical_not(outer))
    def _():
        pl.semaphore_wait(known.at[1], 1)
        tell(2, next_lane)
        to_plane(0, give_e)

    for chunk in range(chunks):
        def spread(g, _, chunk=chunk):
            start = pl.multiple_of(g * group + chunk * SUB, SUB)
            for part in range(2):
                mixed = mix([held[b, part, pl.ds(start, SUB), :] for b in range(blocks)])
                for b in range(blocks):
                    sent1[chunk, b * groups + g, part] = mixed[b]
            return 0

        lax.fori_loop(0, groups, spread, 0)
        swap(sent1.at[chunk], got1.at[chunk], sent.at[1], recv1.at[chunk])
        got1[chunk, me] = sent1[chunk, me]

    arrive(levels, e_recv)

    def phases(d, _):
        c, s = cos_sin(levels[d] * angle_ref[1:2, :])
        cosine[d] = c
        sine[d] = s
        return 0

    lax.fori_loop(0, devices, phases, 0)

    wide = TABLE // SUB
    half = max(chunks // 2, 1)
    thin = (half - 1, chunks - 1) if half > 1 else ()
    fat = [c for c in range(chunks) if c not in thin]
    messages = [(c, ()) for c in fat] + [(c, (h,)) for c in thin for h in range(2)]
    few = blocks // 2

    def give_back(at, far, *some):
        chunk, spot = messages[at]
        ends = sent2.at[chunk], got2.at[chunk], sent.at[2], recv2.at[at]
        to_plane(far, lambda b, l: give(*ends, b, l, spot), *some)

    def send_back(order):
        for at, far, *some in order:
            give_back(at, far, *some)
        for at in sorted({at for at, *_ in order}):
            chunk, spot = messages[at]
            got2[(chunk, me, *spot)] = sent2[(chunk, me, *spot)]

    def far_first(*those):
        return [(at, far) for at in those for far in range(PLANES)]

    def take_back(at):
        chunk, spot = messages[at]
        arrive(got2.at[chunk], recv2.at[at], spot)

    for chunk in range(chunks):
        arrive(got1.at[chunk], recv1.at[chunk])
        if chunk == chunks - 1 > 0:
            pl.when(outer)(lambda: send_back(far_first(0)))
        there = pl.ds(chunk * SUB, SUB)
        re = mix([got1[chunk, d, 0] for d in range(devices)])
        im = mix([got1[chunk, d, 1] for d in range(devices)])
        done = []
        for start in range(0, devices, wide):
            r, i = [], []
            for d in range(start, start + wide):
                c, s = cosine[d, there, :], sine[d, there, :]
                r.append(re[d] * c + im[d] * s)
                i.append(im[d] * c - re[d] * s)
            along = mix_lanes(jnp.concatenate(r + i, axis=0), table)
            pair = jnp.concatenate([along[:TABLE], along[TABLE:]], axis=1)
            high, low = split(pair)
            done.append(dot(table, high) + dot(table, low))
        done = mix(done)
        first = chunk - chunk % half
        last = chunk % half == half - 1
        for d in range(devices):
            at = d % wide * SUB
            for part in range(2):
                tile = done[d // wide][at : at + SUB, part * lanes : (part + 1) * lanes]
                if last:
                    tiles = mix([sent2[c, d, part] for c in range(first, chunk)] + [tile])
                    for c in range(half):
                        sent2[first + c, d, part] = tiles[c]
                else:
                    sent2[chunk, d, part] = tile
        if last and first == chunk + 1 - chunks:
            send_back(far_first(0))
        elif last and first == 0:
            pl.when(jnp.logical_not(outer))(lambda: send_back(far_first(0)))
        elif last:
            send_back(far_first(fat.index(first)))

    for chunk in range(1, half):
        def halves(d, _, chunk=chunk):
            u, v = sent2[chunk, d], sent2[chunk + half, d]
            for to, both in ((chunk, u + v), (chunk + half, u - v)):
                if to in thin:
                    both = [
                        jnp.concatenate([part[h * HALF : (h + 1) * HALF] for part in both])
                        for h in range(2)
                    ]
                for i in range(2):
                    sent2[to, d, i] = both[i]
            return 0

        lax.fori_loop(0, devices, halves, 0)

    scale = float(TABLE * TABLE) / (devices * blocks * rows * lanes)
    share = rows // n_bank // group
    slim = list(range(len(fat), len(messages)))
    steps = [(0, fat.index(half))] if chunks > 1 else [(0,)]
    for first in range(1, half - 1):
        steps += [(fat.index(c),) for c in (first, first + half)]
        send_back(far_first(*steps[-2], *steps[-1]))
    steps += [(at,) for at in slim]
    rows_of = [(far, start, deep // 2) for far in (0, 1) for start in (0, deep // 2)]
    order = [(0, 0), (1, 0), (2, 0), (3, 0), (0, 1), (1, 1), (0, 2), (0, 3), (2, 1), (1, 2), (1, 3), (3, 1), (2, 2), (2, 3), (3, 2), (3, 3)]
    send_back([(at, far) for at in slim for far in (2, 3)])
    if slim:
        send_back([(slim[i], *rows_of[j]) for i, j in order])

    def back(chunk, part):
        return mix([got2[chunk, d, part] for d in range(devices)])

    def whole(step):
        places = [messages[at][0] for at in step]
        for at, chunk in zip(step[:-1], places):
            take_back(at)
            for part in range(2):
                mixed = back(chunk, part)
                for d in range(devices):
                    got2[chunk, d, part] = mixed[d]
        take_back(step[-1])
        for part in range(2):
            mixed = back(places[-1], part)
            for d in range(devices):
                tiles = mix([got2[c, d, part] for c in places[:-1]] + [mixed[d]])
                b, g = divmod(d, groups)
                for at, chunk, tile in zip(step, places, tiles):
                    value = tile * scale
                    row = g * group + chunk * SUB
                    out_ref[part, b, row : row + SUB, :] = value
                    spot = (at, g // share, b, pl.ds(g % share * SUB, SUB))
                    square = value * value
                    chance[spot] = chance[spot] + square if part else square

    def thinner(at):
        take_back(at)
        chunk, (h,) = messages[at]
        mixed = back(chunk, h)
        for d in range(devices):
            b, g = divmod(d, groups)
            value = mixed[d] * scale
            row = g * group + chunk * SUB + h * HALF
            for part in range(2):
                out_ref[part, b, row : row + HALF, :] = value[part * HALF : (part + 1) * HALF]
            square = value * value
            low, high = b % few, b // few
            spot = (at - len(fat), g // share, low, pl.ds(g % share * SUB + high * HALF, HALF))
            thin_chance[spot] = square[:HALF] + square[HALF:]

    for step in steps:
        if step[0] < len(fat):
            whole(step)
        else:
            thinner(step[0])
        for at in step:
            src, dst, place, group_sem = chance, chances, at, 3
            if at >= len(fat):
                src, dst, place, group_sem = thin_chance, thin_chances, at - len(fat), 4
            for turn in range(1, n_bank):
                other = lax.rem(bank + turn, n_bank)
                pltpu.make_async_remote_copy(
                    src_ref=src.at[place, other], dst_ref=dst.at[place, turn - 1],
                    send_sem=sent.at[group_sem], recv_sem=m_recv.at[group_sem - 3],
                    device_id=(other, lane), device_id_type=MESH,
                ).start()
    wait_for(chances, m_recv.at[0])
    if slim:
        wait_for(thin_chances, m_recv.at[1])
    for step in steps:
        for at in step:
            src, dst, place = chance, chances, at
            if at >= len(fat):
                src, dst, place = thin_chance, thin_chances, at - len(fat)
            total = src[place, bank]
            for turn in range(1, n_bank):
                total = total + dst[place, turn - 1]
            total = total * (1.0 / n_bank)
            chunk, spot = messages[at]
            for g in range(share):
                row = g * group + chunk * SUB
                if not spot:
                    marginal_ref[:, row : row + SUB, :] = total[:, g * SUB : (g + 1) * SUB]
                    continue
                row = row + spot[0] * HALF
                for high in range(2):
                    at_row = g * SUB + high * HALF
                    marginal_ref[high * few : (high + 1) * few, row : row + HALF, :] = (
                        total[:, at_row : at_row + HALF]
                    )

    wait_for(chances, sent.at[3])
    if slim:
        wait_for(thin_chances, sent.at[4])
    arrive(e_ref, sent.at[0])
    wait_for(sent1.at[:, pl.ds(0, devices - 1)], sent.at[1])
    wait_for(sent2.at[:, pl.ds(0, devices - 1)], sent.at[2])


def put_out(state_ref, marginal_ref, state_out, marginal_out, sem):
    copies = [
        pltpu.make_async_copy(state_ref, state_out, sem.at[0]),
        pltpu.make_async_copy(marginal_ref, marginal_out, sem.at[1]),
    ]
    for copy in copies:
        copy.start()
    for copy in copies:
        copy.wait()


def shards(n_bank, n_lane, amplitudes, energies, angles):
    devices = n_bank * n_lane
    _, blocks, rows, lanes = amplitudes.shape
    group = blocks * rows // devices
    chunks = group // SUB
    f32 = jnp.float32
    whole = pl.BlockSpec(memory_space=pltpu.VMEM)
    swapped = pltpu.VMEM((chunks, devices, 2, SUB, lanes), f32)
    real = pltpu.VMEM((devices, group, lanes), f32)
    strip = (blocks, rows // n_bank, lanes)
    part = (blocks, rows // n_bank // chunks, lanes)
    thin = (blocks // 2, rows // n_bank // chunks, lanes)
    n_thin = 4 if chunks > 2 else 0
    n_fat = chunks - n_thin // 2
    n_messages = n_fat + n_thin
    more = pltpu.SemaphoreType.DMA((n_messages,))
    state, marginal = pl.pallas_call(
        functools.partial(kernel, n_bank, n_lane, chunks),
        out_shape=(
            pltpu.VMEM(amplitudes.shape, f32),
            pltpu.VMEM(strip, f32),
        ),
        in_specs=[pl.BlockSpec(memory_space=pltpu.HBM)] * 3,
        out_specs=(whole, whole),
        scratch_shapes=[
            pltpu.VMEM(amplitudes.shape, f32),
            real,
            pltpu.VMEM(angles.shape, f32),
            pltpu.VMEM((TABLE, TABLE), jnp.bfloat16),
            pltpu.VMEM((blocks, 2, rows, lanes), f32),
            swapped, swapped, swapped, swapped,
            real, real, real,
            pltpu.VMEM((n_fat, n_bank, *part), f32),
            pltpu.VMEM((n_fat, n_bank - 1, *part), f32),
            pltpu.VMEM((max(n_thin, 1), n_bank, *thin), f32),
            pltpu.VMEM((max(n_thin, 1), n_bank - 1, *thin), f32),
            pltpu.SemaphoreType.DMA((3,)),
            pltpu.SemaphoreType.DMA((5,)),
            pltpu.SemaphoreType.DMA,
            pltpu.SemaphoreType.DMA((chunks,)),
            more,
            pltpu.SemaphoreType.DMA((2,)),
            pltpu.SemaphoreType.REGULAR((4,)),
        ],
        compiler_params=pltpu.CompilerParams(
            collective_id=0, has_side_effects=True
        ),
        name="walsh",
    )(amplitudes, energies.reshape(devices, group, lanes), angles)
    return pl.pallas_call(
        put_out,
        out_shape=(
            jax.ShapeDtypeStruct(state.shape, f32),
            jax.ShapeDtypeStruct(marginal.shape, f32),
        ),
        in_specs=[whole] * 2,
        out_specs=(pl.BlockSpec(memory_space=pltpu.HBM),) * 2,
        scratch_shapes=[pltpu.SemaphoreType.DMA((2,))],
        compiler_params=pltpu.CompilerParams(vmem_limit_bytes=1024 * 1024),
        name="put_out",
    )(state, marginal)


def solution(mesh):
    sizes = mesh.shape
    return jax.shard_map(
        functools.partial(shards, sizes["bank"], sizes["lane"]),
        mesh=mesh,
        in_specs=(P(None, ("bank", "lane"), None, None), P(("bank", "lane"), None, None), P()),
        out_specs=(P(None, ("bank", "lane"), None, None), P("lane", "bank", None)),
        check_vma=False,
    )
```
